32 devices in a mesh: pairs: 16 (over z, y, x), comp: 2 (over core).
Axes of the slice: x: 2, y: 2, z: 4, core: 2. Of those that a mesh axis runs over, the one named last changes fastest.
Arguments:
- effects: float32 [49, 131072], P(None, 'pairs'), may hold values from -24 to 24
- se_table: float32 [16, 49], replicated, may hold values from 0.5 to 2
- se_index: int32 [256], P('pairs'), may hold values from 0 to 15
- base_root: float32 [16, 49, 49], replicated, may hold values from -0.875 to 0.875
- grid_scale: float32 [16], replicated, may hold values from 0.25 to 4
- comp_base: int32 [256], P('comp'), may hold values from 0 to 15
- comp_grid: int32 [256], P('comp'), may hold values from 0 to 15
- weights: float32 [256], P('comp'), may hold values from 0.2 to 5
Outputs:
- responsibility: float32 [256, 131072], P('comp', 'pairs')
- log_weights: float32 [256], P('comp')
- pair_loglik: float32 [131072], P('pairs')
The draws below stay inside these ranges and needn't reach their ends.
All inputs are finite; a program needn't handle non-finite values.
Results may differ from the reference program's by a relative error of at most 0.0003.
Values sent between devices are 32-bit elements; how exact they have to be, the bound alone decides.
No kernel may reach another device: no remote copies, remote signals or barrier semaphores. Data moves between devices by JAX's collectives and lax.ppermute only.
A program may use at most 384 MiB of HBM per device.

```python
import math
import jax
import jax.numpy as jnp
from jax import lax

R = 49
NU = 16
NGRID = 16
NB = 16
TILE = 512
PAIRS = 131072
K = 256


def draw_effects(key, part):
    key_scale, key_base, key_flag, key_sign = jax.random.split(key, 4)
    values = 1.5 * jax.random.normal(key_base, (R, PAIRS), dtype=jnp.float32)
    return jnp.clip(values, -8.0, 8.0).astype(jnp.float32)


def plant(entries, rng, low, top_value):
    longest = entries.shape.index(max(entries.shape))
    spots = []
    for shift in (0, 1):
        where = [jax.random.randint(jax.random.fold_in(rng, axis), (), 0, length) for axis, length in enumerate(entries.shape)]
        where[longest] = (where[longest] + shift) % entries.shape[longest]
        spots.append(tuple(where))
    return entries.at[spots[0]].set(low).at[spots[1]].set(top_value)


def steps_of(stream_key, extent, pieces, least, top_value):
    gain, own = 1.0, jax.random.fold_in(stream_key, 6)
    for axis_at, blocks in pieces:
        heights = jnp.exp(jax.random.uniform(jax.random.fold_in(own, axis_at), (blocks,), jnp.float32, least / len(pieces), top_value / len(pieces)))
        gain = gain * jnp.repeat(heights, extent[axis_at] // blocks).reshape([-1 if axis == axis_at else 1 for axis in range(len(extent))])
    return gain


def normal_values(stream_key, shape, deviation, most, kind=jnp.bfloat16):
    return jnp.clip(deviation * jax.random.normal(stream_key, shape, jnp.float32), -most, most).astype(kind)


def setup_inputs(seed: int = 0) -> dict:
    arg_keys = jax.random.split(jax.random.key(seed), 9)
    return {
        "effects": draw_effects(jax.random.fold_in(arg_keys[8], 71), 0),
        "se_table": jnp.clip(jnp.exp(jax.random.uniform(arg_keys[1], (NB, R), jnp.float32, math.log(0.5), math.log(2.0))), 0.5, 2.0),
        "se_index": plant(jax.random.randint(arg_keys[2], (PAIRS // TILE,), 0, NB), jax.random.fold_in(arg_keys[2], 1), 0, NB - 1).astype(jnp.int32),
        "base_root": normal_values(arg_keys[3], (NU, R, R), R ** -0.5, 0.875, jnp.float32),
        "grid_scale": jnp.clip(jnp.exp(jax.random.uniform(arg_keys[4], (NGRID,), jnp.float32, math.log(0.25), math.log(4.0))), 0.25, 4.0),
        "comp_base": plant(jax.random.randint(arg_keys[5], (K,), 0, NU), jax.random.fold_in(arg_keys[5], 1), 0, NU - 1).astype(jnp.int32),
        "comp_grid": plant(jax.random.randint(arg_keys[6], (K,), 0, NGRID), jax.random.fold_in(arg_keys[6], 1), 0, NGRID - 1).astype(jnp.int32),
        "weights": jnp.clip(jnp.exp(math.log(5.0) - 3.218876 * jax.random.uniform(arg_keys[7], (K,), jnp.float32) ** steps_of(arg_keys[7], (K,), ((0, 2),), -0.2, 0.2)), 0.2, 5.0),
    }


def whiten_tables(se_table, base_root, grid_scale, comp_base, comp_grid):
    covariances = jnp.einsum('uij,ukj->uik', base_root, base_root, precision=lax.Precision.HIGHEST)
    picked = covariances[comp_base]
    scales = grid_scale[comp_grid]
    identity = jnp.eye(R, dtype=base_root.dtype)
    system = (scales * scales)[None, :, None, None] * picked[None]
    system = system + identity[None, None] * (se_table * se_table)[:, None, :, None]
    factor = jnp.linalg.cholesky(system)
    eye_full = jnp.broadcast_to(identity, factor.shape)
    inverse = jax.scipy.linalg.solve_triangular(factor, eye_full, lower=True)
    half_logdet = jnp.sum(jnp.log(jnp.diagonal(factor, axis1=2, axis2=3)), axis=-1)
    return (inverse, half_logdet)

def reference(effects, se_table, se_index, base_root, grid_scale, comp_base, comp_grid, weights):
    inverse, half_logdet = whiten_tables(se_table, base_root, grid_scale, comp_base, comp_grid)
    log_prior = jnp.log(weights)
    constant = 0.5 * R * math.log(2.0 * math.pi)
    tile_rows = effects.reshape(R, PAIRS // TILE, TILE).transpose(1, 0, 2)

    def one_tile(inputs):
        block_id, tile_data = inputs
        whitened = jnp.einsum('kij,jp->kip', inverse[block_id], tile_data, precision=lax.Precision.HIGHEST)
        quadratic = jnp.sum(whitened * whitened, axis=1)
        return log_prior[:, None] - 0.5 * quadratic - half_logdet[block_id][:, None] - constant
    scores = lax.map(one_tile, (se_index.astype(jnp.int32), tile_rows))
    scores = scores.transpose(1, 0, 2).reshape(K, PAIRS)
    score_max = jnp.max(scores, axis=0)
    score_sum = jnp.sum(jnp.exp(scores - score_max), axis=0)
    pair_loglik = score_max + jnp.log(score_sum)
    responsibility = jnp.exp(scores - pair_loglik)
    masses = jnp.sum(responsibility, axis=1)
    log_weights = jnp.log((masses + 1.0) / (PAIRS + K))
    return (responsibility, log_weights, pair_loglik)
```

```python
import functools
import math

import jax
import jax.numpy as jnp
from jax import lax
from jax.experimental import pallas as pl
from jax.experimental.pallas import tpu as pltpu
from jax.sharding import PartitionSpec as P

TILE = 512
SUB = 8
LANES = 128
PIECES = 5


def block_edge(count):
    return max(edge for edge in range(1, 9) if count % edge == 0)


def element(index):
    return pl.ds(pl.multiple_of(index * SUB, SUB), SUB)


def eliminate(n, table, pivots, factors):
    edge = block_edge(n)
    blocks = n // edge

    def at(i, j):
        return element(i * n + j)

    def one_pivot_block(kb, carry):
        first = kb * edge
        diag = [[table[at(first + m, first + j), :] if j >= m else None for j in range(edge)] for m in range(edge)]
        lower = [[None] * edge for _ in range(edge)]
        inverse = [[None] * edge for _ in range(edge)]
        recips = []
        for m in range(edge):
            d = diag[m][m]
            recip = 1.0 / d
            recips.append(recip)
            pivots[element(first + m), :] = d
            for r in range(m + 1, edge):
                lower[r][m] = diag[m][r] * recip
            for r in range(m + 1, edge):
                for j in range(r, edge):
                    diag[r][j] = diag[r][j] - lower[r][m] * diag[m][j]
                for j in range(m):
                    inverse[r][j] = inverse[r][j] - lower[r][m] * inverse[m][j]
                inverse[r][m] = -lower[r][m]
        for r in range(edge):
            for j in range(r):
                table[at(first + r, first + j), :] = inverse[r][j]

        def column_block(jb, with_factor):
            col = jb * edge
            for j in range(edge):
                rows = [table[at(first + m, col + j), :] for m in range(edge)]
                for m in range(edge):
                    for r in range(m + 1, edge):
                        rows[r] = rows[r] - lower[r][m] * rows[m]
                for m in range(edge):
                    if m:
                        table[at(first + m, col + j), :] = rows[m]
                    if with_factor:
                        factors[element(m * n + col + j), :] = rows[m] * recips[m]

        def left(jb, c):
            column_block(jb, False)
            return c

        def right(jb, c):
            column_block(jb, True)
            return c

        lax.fori_loop(0, kb, left, 0)
        lax.fori_loop(kb + 1, blocks, right, 0)

        def row_block(ib, c):
            row = ib * edge
            for i in range(edge):
                f = [factors[element(m * n + row + i), :] for m in range(edge)]
                for j in range(edge):
                    total = f[j]
                    for m in range(j + 1, edge):
                        total = total + f[m] * inverse[m][j]
                    table[at(row + i, first + j), :] = -total

            for i in range(edge):
                f = [factors[element(m * n + row + i), :] for m in range(edge)]
                for j in range(i, edge):
                    value = table[at(row + i, row + j), :]
                    for m in range(edge):
                        value = value - f[m] * table[at(first + m, row + j), :]
                    table[at(row + i, row + j), :] = value

            def full(index, cc):
                jb = jnp.where(index < kb, index, index - kb + ib + 1)
                col = jb * edge
                start = 0
                for size in (edge - edge // 2, edge // 2):
                    rows = range(start, start + size)
                    start += size
                    held = [[table[at(row + i, col + j), :] for j in range(edge)] for i in rows]
                    for m in range(edge):
                        f = [factors[element(m * n + row + i), :] for i in rows]
                        for j in range(edge):
                            u = table[at(first + m, col + j), :]
                            for a in range(len(f)):
                                held[a][j] = held[a][j] - f[a] * u
                    for a, i in enumerate(rows):
                        for j in range(edge):
                            table[at(row + i, col + j), :] = held[a][j]
                return cc

            lax.fori_loop(0, kb + blocks - 1 - ib, full, 0)
            return c

        lax.fori_loop(kb + 1, blocks, row_block, 0)
        return carry

    lax.fori_loop(0, blocks, one_pivot_block, 0)


def split3(value):
    one = value.astype(jnp.bfloat16)
    rest = value - one.astype(jnp.float32)
    two = rest.astype(jnp.bfloat16)
    three = (rest - two.astype(jnp.float32)).astype(jnp.bfloat16)
    return one, two, three


def main_kernel(
    n, tiles, patterns,
    index_ref, effects_ref, se_ref, covar_ref, prior_ref,
    out_ref, max_ref, sum_ref,
    table, pivots, factors, roots, halfdet, noise, weights, flipped, stack, acc, se_rows,
    count_s, start_s, slot_s, order_s,
):
    comps = LANES
    even = n // 16 * 16
    edge_rows = n - even

    def clear(b, c):
        count_s[b] = 0
        return c

    lax.fori_loop(0, patterns, clear, 0)

    def tally(t, c):
        b = index_ref[t]
        count_s[b] = count_s[b] + 1
        return c

    lax.fori_loop(0, tiles, tally, 0)

    def place(b, state):
        used, offset = state
        many = count_s[b]
        slot_s[used] = b
        start_s[used] = offset
        count_s[b] = offset
        return used + jnp.where(many > 0, 1, 0), offset + many

    used, _ = lax.fori_loop(0, patterns, place, (jnp.int32(0), jnp.int32(0)))
    start_s[used] = tiles

    def sort(t, c):
        b = index_ref[t]
        position = count_s[b]
        order_s[position] = t
        count_s[b] = position + 1
        return c

    lax.fori_loop(0, tiles, sort, 0)

    weights[...] = jnp.zeros_like(weights)
    stack[...] = jnp.zeros_like(stack)

    def one_batch(batch, carry):
        base = batch * SUB
        for s in range(SUB):
            b = slot_s[jnp.minimum(base + s, used - 1)]
            se_rows[pl.ds(s, 1), :] = se_ref[pl.ds(b, 1), :]
        ses = se_rows[...]
        squares = ses * ses
        for i in range(n):
            noise[pl.ds(i * SUB, SUB), :] = jnp.broadcast_to(squares[:, i : i + 1], (SUB, LANES))

        def fill_row(i, c):
            def fill(j, cc):
                e = i * n + j
                table[element(e), :] = covar_ref[pl.ds(e, SUB, stride=0), :]
                return cc

            def fill_block(jb, cc):
                for a in range(block_edge(n)):
                    fill(jb * block_edge(n) + a, 0)
                return cc

            lax.fori_loop(i // block_edge(n), n // block_edge(n), fill_block, 0)
            d = element(i * n + i)
            table[d, :] = table[d, :] + noise[element(i), :]
            return c

        lax.fori_loop(0, n, fill_row, 0)
        eliminate(n, table, pivots, factors)
        logs = jnp.zeros((SUB, LANES), jnp.float32)
        for i in range(n):
            d = pivots[pl.ds(i * SUB, SUB), :]
            roots[pl.ds(i * SUB, SUB), :] = lax.rsqrt(d)
            logs = logs + jnp.log(d)
        halfdet[...] = prior_ref[...] - 0.5 * logs

        def one_slot(slot, c):
            s = slot - base
            for i in range(n):
                groups = min(i // 16 + 1, even // 16)
                rows = groups * 16
                root = roots[pl.ds(i * SUB + s, SUB, stride=0), :][0:1, :]
                row = table[pl.ds(i * n * SUB + s, rows, stride=SUB), :]
                if i < even:
                    j = lax.broadcasted_iota(jnp.int32, (rows, LANES), 0)
                    row = jnp.where(j < i, row, jnp.where(j == i, 1.0, 0.0))
                row = row * root
                one = row.astype(jnp.bfloat16)
                two = (row - one.astype(jnp.float32)).astype(jnp.bfloat16)
                for piece, part in enumerate((one, one, two, two, one)):
                    weights[i, pl.ds(piece * even, rows), :] = part
                if i >= even:
                    first = root.astype(jnp.bfloat16)
                    second = (root - first.astype(jnp.float32)).astype(jnp.bfloat16)
                    j = lax.broadcasted_iota(jnp.int32, (16, LANES), 0)
                    tail = jnp.zeros((16, LANES), jnp.float32)
                    for piece, part in enumerate((first, first, second, second, first)):
                        tail = jnp.where(j == piece, part.astype(jnp.float32), tail)
                    weights[i, pl.ds(PIECES * even, 16), :] = tail.astype(jnp.bfloat16)
            row_const = halfdet[pl.ds(s, 1), :]

            def one_tile(place_at, cc):
                t = order_s[place_at]
                at = pl.ds(pl.multiple_of(t * TILE, TILE), TILE)
                data = effects_ref[pl.ds(0, even), at]
                x1, x2, x3 = split3(data)
                for piece, part in enumerate((x1, x2, x1, x2, x3)):
                    stack[pl.ds(piece * even, even), :] = part.astype(jnp.float32)
                for extra in range(edge_rows):
                    line = effects_ref[pl.ds(even + extra, 1), at]
                    x1, x2, x3 = split3(line)
                    for piece, part in enumerate((x1, x2, x1, x2, x3)):
                        stack[pl.ds(PIECES * even + extra * PIECES + piece, 1), :] = part.astype(jnp.float32)
                flipped[...] = jnp.transpose(stack[...]).astype(jnp.bfloat16)
                for i in range(0, n, 2):
                    if i + 1 < n:
                        right = jnp.concatenate([weights[i], weights[i + 1]], axis=1)
                    else:
                        right = weights[i]
                    white = jnp.dot(flipped[...], right, preferred_element_type=jnp.float32)
                    square = white[:, :LANES] * white[:, :LANES]
                    if i + 1 < n:
                        square = square + white[:, LANES:] * white[:, LANES:]
                    if i:
                        acc[...] += square
                    else:
                        acc[...] = square
                scores = jnp.transpose(row_const - 0.5 * acc[...])
                top = jnp.max(scores, axis=0, keepdims=True)
                shifted = jnp.exp(scores - top)
                out_ref[:, at] = shifted
                max_ref[:, at] = top
                sum_ref[:, at] = jnp.sum(shifted, axis=0, keepdims=True)
                return cc

            lax.fori_loop(start_s[slot], start_s[slot + 1], one_tile, 0)
            return c

        lax.fori_loop(base, jnp.minimum(used, base + SUB), one_slot, 0)
        return carry

    lax.fori_loop(0, (used + SUB - 1) // SUB, one_batch, 0)


def shifted_scores(effects, se_table, se_index, covar, prior):
    n, pairs = effects.shape
    patterns = se_table.shape[0]
    tiles = pairs // TILE
    even = n // 16 * 16
    assert covar.shape == (n * n, LANES) and (n - even) * PIECES <= 16
    depth = PIECES * even + 16
    se_wide = jnp.pad(se_table, ((0, 0), (0, LANES - n)))
    vmem = pl.BlockSpec(memory_space=pltpu.VMEM)
    smem = pl.BlockSpec(memory_space=pltpu.SMEM)
    f32 = jnp.float32
    return pl.pallas_call(
        functools.partial(main_kernel, n, tiles, patterns),
        name="shifted_scores",
        out_shape=(
            jax.ShapeDtypeStruct((LANES, pairs), f32),
            jax.ShapeDtypeStruct((1, pairs), f32),
            jax.ShapeDtypeStruct((1, pairs), f32),
        ),
        in_specs=[smem, vmem, vmem, vmem, vmem],
        out_specs=(vmem, vmem, vmem),
        scratch_shapes=[
            pltpu.VMEM((n * n * SUB, LANES), f32),
            pltpu.VMEM((n * SUB, LANES), f32),
            pltpu.VMEM((block_edge(n) * n * SUB, LANES), f32),
            pltpu.VMEM((n * SUB, LANES), f32),
            pltpu.VMEM((SUB, LANES), f32),
            pltpu.VMEM((n * SUB, LANES), f32),
            pltpu.VMEM((n, depth, LANES), jnp.bfloat16),
            pltpu.VMEM((TILE, depth), jnp.bfloat16),
            pltpu.VMEM((depth, TILE), f32),
            pltpu.VMEM((TILE, LANES), f32),
            pltpu.VMEM((SUB, LANES), f32),
            pltpu.SMEM((patterns + 1,), jnp.int32),
            pltpu.SMEM((patterns + 1,), jnp.int32),
            pltpu.SMEM((patterns + 1,), jnp.int32),
            pltpu.SMEM((tiles,), jnp.int32),
        ],
        compiler_params=pltpu.CompilerParams(vmem_limit_bytes=60 * 1024 * 1024),
    )(se_index, effects, se_wide, covar, prior)


def exact_dot(left, right, dims):
    return lax.dot_general(left, right, (dims, ((), ())), precision=lax.Precision.HIGHEST, preferred_element_type=jnp.float32)


def finish_kernel(shifted_ref, scale_ref, out_ref, mass_ref):
    value = shifted_ref[...] * scale_ref[...]
    out_ref[...] = value
    total = jnp.sum(value, axis=1, keepdims=True)

    @pl.when(pl.program_id(0) == 0)
    def _():
        mass_ref[...] = jnp.zeros_like(mass_ref)

    mass_ref[...] += total


def finish(shifted, scale):
    comps, pairs = shifted.shape
    width = min(pairs, 1024)
    return pl.pallas_call(
        finish_kernel,
        name="finish",
        grid=(pairs // width,),
        in_specs=[
            pl.BlockSpec((comps, width), lambda g: (0, g)),
            pl.BlockSpec((1, width), lambda g: (0, g)),
        ],
        out_specs=(
            pl.BlockSpec((comps, width), lambda g: (0, g)),
            pl.BlockSpec((comps, 1), lambda g: (0, 0)),
        ),
        out_shape=(
            jax.ShapeDtypeStruct((comps, pairs), jnp.float32),
            jax.ShapeDtypeStruct((comps, 1), jnp.float32),
        ),
    )(shifted, scale)


def per_device(effects, se_table, se_index, base_root, grid_scale, comp_base, comp_grid, weights):
    n, pairs = effects.shape
    comps = comp_base.shape[0]
    covariances = jnp.einsum("uij,ukj->uik", base_root, base_root, precision=lax.Precision.HIGHEST)
    covariances = covariances.reshape(covariances.shape[0], n * n)
    bases = jnp.arange(covariances.shape[0], dtype=jnp.int32)
    grids = jnp.arange(grid_scale.shape[0], dtype=jnp.int32)
    scale = jnp.sum(jnp.where(comp_grid[None] == grids[:, None], grid_scale[:, None], 0.0), axis=0)
    pick = (comp_base[None] == bases[:, None]).astype(jnp.float32)
    covar = exact_dot(covariances, pick, ((0,), (0,))) * (scale * scale)[None]
    prior = (jnp.log(weights) - 0.5 * n * math.log(2.0 * math.pi))[None]
    shifted, top, total = shifted_scores(effects, se_table, se_index, covar, prior)
    both = lax.all_gather(jnp.concatenate([top, total], axis=0), "comp")
    tops, totals = both[:, 0], both[:, 1]
    score_max = jnp.max(tops, axis=0)
    score_sum = jnp.sum(totals * jnp.exp(tops - score_max), axis=0)
    pair_loglik = score_max + jnp.log(score_sum)
    responsibility, mass = finish(shifted, jnp.exp(top - pair_loglik[None]))
    masses = lax.psum(mass[:, 0], "pairs")
    all_pairs = pairs * lax.axis_size("pairs")
    all_comps = comps * lax.axis_size("comp")
    log_weights = jnp.log((masses + 1.0) / (all_pairs + all_comps))
    return (responsibility, log_weights, pair_loglik)


def solution(mesh):
    placed = (P(None, "pairs"), P(), P("pairs"), P(), P(), P("comp"), P("comp"), P("comp"))
    return jax.shard_map(
        per_device,
        mesh=mesh,
        in_specs=placed,
        out_specs=(P("comp", "pairs"), P("comp"), P("pairs")),
        check_vma=False,
    )
```

```python
import functools
import math

import jax
import jax.numpy as jnp
from jax import lax
from jax.experimental import pallas as pl
from jax.experimental.pallas import tpu as pltpu
from jax.sharding import PartitionSpec as P

TILE = 512
SUB = 8
LANES = 128
PIECES = 5


def block_edge(count):
    return max(edge for edge in range(1, 9) if count % edge == 0)


def element(index):
    return pl.ds(pl.multiple_of(index * SUB, SUB), SUB)


def eliminate(n, table, pivots, factors):
    edge = block_edge(n)
    blocks = n // edge

    def at(i, j):
        return element(i * n + j)

    def one_pivot_block(kb, carry):
        first = kb * edge
        diag = [[table[at(first + m, first + j), :] if j >= m else None for j in range(edge)] for m in range(edge)]
        lower = [[None] * edge for _ in range(edge)]
        inverse = [[None] * edge for _ in range(edge)]
        recips = []
        for m in range(edge):
            d = diag[m][m]
            recip = 1.0 / d
            recips.append(recip)
            pivots[element(first + m), :] = d
            for r in range(m + 1, edge):
                lower[r][m] = diag[m][r] * recip
            for r in range(m + 1, edge):
                for j in range(r, edge):
                    diag[r][j] = diag[r][j] - lower[r][m] * diag[m][j]
                for j in range(m):
                    inverse[r][j] = inverse[r][j] - lower[r][m] * inverse[m][j]
                inverse[r][m] = -lower[r][m]
        for r in range(edge):
            for j in range(r):
                table[at(first + r, first + j), :] = inverse[r][j]

        def column_block(jb, with_factor):
            col = jb * edge
            for j in range(edge):
                rows = [table[at(first + m, col + j), :] for m in range(edge)]
                for m in range(edge):
                    for r in range(m + 1, edge):
                        rows[r] = rows[r] - lower[r][m] * rows[m]
                for m in range(edge):
                    if m:
                        table[at(first + m, col + j), :] = rows[m]
                    if with_factor:
                        factors[element(m * n + col + j), :] = rows[m] * recips[m]

        def left(jb, c):
            column_block(jb, False)
            return c

        def right(jb, c):
            column_block(jb, True)
            return c

        lax.fori_loop(0, kb, left, 0)
        lax.fori_loop(kb + 1, blocks, right, 0)

        def row_block(ib, c):
            row = ib * edge
            start = 0
            for size in (edge - edge // 2, edge // 2):
                rows = range(start, start + size)
                start += size
                f = [[factors[element(m * n + row + i), :] for m in range(edge)] for i in rows]
                for j in range(edge):
                    totals = [f[a][j] for a in range(size)]
                    for m in range(j + 1, edge):
                        v = table[at(first + m, first + j), :]
                        totals = [totals[a] + f[a][m] * v for a in range(size)]
                    for a, i in enumerate(rows):
                        table[at(row + i, first + j), :] = -totals[a]
                for j in range(rows[0], edge):
                    live = [a for a, i in enumerate(rows) if i <= j]
                    values = [table[at(row + rows[a], row + j), :] for a in live]
                    for m in range(edge):
                        u = table[at(first + m, row + j), :]
                        values = [v - f[a][m] * u for a, v in zip(live, values)]
                    for a, v in zip(live, values):
                        table[at(row + rows[a], row + j), :] = v

            def full(index, cc):
                jb = jnp.where(index < kb, index, index - kb + ib + 1)
                col = jb * edge
                start = 0
                for size in (edge - edge // 2, edge // 2):
                    rows = range(start, start + size)
                    start += size
                    held = [[table[at(row + i, col + j), :] for j in range(edge)] for i in rows]
                    for m in range(edge):
                        f = [factors[element(m * n + row + i), :] for i in rows]
                        for j in range(edge):
                            u = table[at(first + m, col + j), :]
                            for a in range(len(f)):
                                held[a][j] = held[a][j] - f[a] * u
                    for a, i in enumerate(rows):
                        for j in range(edge):
                            table[at(row + i, col + j), :] = held[a][j]
                return cc

            lax.fori_loop(0, kb + blocks - 1 - ib, full, 0)
            return c

        lax.fori_loop(kb + 1, blocks, row_block, 0)
        return carry

    lax.fori_loop(0, blocks, one_pivot_block, 0)


def split3(value):
    one = value.astype(jnp.bfloat16)
    rest = value - one.astype(jnp.float32)
    two = rest.astype(jnp.bfloat16)
    three = (rest - two.astype(jnp.float32)).astype(jnp.bfloat16)
    return one, two, three


def main_kernel(
    n, tiles, patterns, grids,
    index_ref, grid_ref, effects_hbm, se_ref, covar_ref, comp_grid_ref, prior_ref,
    out_hbm, peak_ref,
    table, pivots, factors, roots, halfdet, noise, weights, effects_ref, flipped, following, stack, acc, done, out_buf, se_rows,
    in_sem, out_sem,
    count_s, start_s, slot_s, order_s,
):
    even = n // 16 * 16
    edge_rows = n - even
    edge = block_edge(n)
    fetch = pltpu.make_async_copy(effects_hbm, effects_ref, in_sem)
    fetch.start()

    def clear(b, c):
        count_s[b] = 0
        return c

    lax.fori_loop(0, patterns, clear, 0)

    def tally(t, c):
        b = index_ref[t]
        count_s[b] = count_s[b] + 1
        return c

    lax.fori_loop(0, tiles, tally, 0)

    def place(b, state):
        used, offset = state
        many = count_s[b]
        slot_s[used] = b
        start_s[used] = offset
        count_s[b] = offset
        return used + jnp.where(many > 0, 1, 0), offset + many

    used, _ = lax.fori_loop(0, patterns, place, (jnp.int32(0), jnp.int32(0)))
    start_s[used] = tiles

    def sort(t, c):
        b = index_ref[t]
        position = count_s[b]
        order_s[position] = t
        count_s[b] = position + 1
        return c

    lax.fori_loop(0, tiles, sort, 0)
    order_s[tiles] = 0

    weights[...] = jnp.zeros_like(weights)
    stack[...] = jnp.zeros_like(stack)
    chosen = comp_grid_ref[...]
    scale = jnp.zeros(chosen.shape, jnp.float32)
    for g in range(grids):
        scale = jnp.where(chosen == g, grid_ref[g], scale)
    scale = jnp.broadcast_to(scale * scale, (SUB, LANES))
    log_prior = jnp.log(prior_ref[...]) - 0.5 * n * math.log(2.0 * math.pi)

    def columns(t):
        return pl.ds(pl.multiple_of(t * TILE, TILE), TILE)

    def prepare(t, target):
        at = columns(t)
        data = effects_ref[pl.ds(0, even), at]
        x1, x2, x3 = split3(data)
        for piece, part in enumerate((x1, x2, x1, x2, x3)):
            stack[pl.ds(piece * even, even), :] = part.astype(jnp.float32)
        for extra in range(edge_rows):
            line = effects_ref[pl.ds(even + extra, 1), at]
            x1, x2, x3 = split3(line)
            for piece, part in enumerate((x1, x2, x1, x2, x3)):
                stack[pl.ds(PIECES * even + extra * PIECES + piece, 1), :] = part.astype(jnp.float32)
        target[...] = jnp.transpose(stack[...]).astype(jnp.bfloat16)

    def conclude(t, side):
        at = columns(t)
        scores = jnp.transpose(done[...])
        top = jnp.max(scores, axis=0, keepdims=True)
        shifted = jnp.exp(scores - top)
        out_buf[side] = shifted
        peak_ref[0:1, at] = top
        peak_ref[1:2, at] = jnp.sum(shifted, axis=0, keepdims=True)

    def store(t, side):
        return pltpu.make_async_copy(out_buf.at[side], out_hbm.at[:, columns(t)], out_sem.at[side])

    def one_batch(batch, carry):
        base = batch * SUB
        for s in range(SUB):
            b = slot_s[jnp.minimum(base + s, used - 1)]
            se_rows[pl.ds(s, 1), :] = se_ref[pl.ds(b, 1), :]
        ses = se_rows[...]
        squares = ses * ses
        for i in range(n):
            noise[pl.ds(i * SUB, SUB), :] = jnp.broadcast_to(squares[:, i : i + 1], (SUB, LANES))

        for rb in range(n // edge):
            def fill_row(i, c):
                for j in range(rb * edge, n):
                    e = i * n + j
                    table[element(e), :] = covar_ref[pl.ds(e, SUB, stride=0), :] * scale
                d = element(i * n + i)
                table[d, :] = table[d, :] + noise[element(i), :]
                return c

            lax.fori_loop(rb * edge, (rb + 1) * edge, fill_row, 0)
        eliminate(n, table, pivots, factors)
        logs = jnp.zeros((SUB, LANES), jnp.float32)
        for i in range(n):
            d = pivots[pl.ds(i * SUB, SUB), :]
            roots[pl.ds(i * SUB, SUB), :] = lax.rsqrt(d)
            logs = logs + jnp.log(d)
        halfdet[...] = log_prior - 0.5 * logs

        @pl.when(batch == 0)
        def _():
            fetch.wait()
            prepare(order_s[0], following)

        def one_slot(slot, c):
            s = slot - base
            for i in range(n):
                groups = min(i // 16 + 1, even // 16)
                rows = groups * 16
                root = roots[pl.ds(i * SUB + s, SUB, stride=0), :][0:1, :]
                row = table[pl.ds(i * n * SUB + s, rows, stride=SUB), :]
                if i < even:
                    j = lax.broadcasted_iota(jnp.int32, (rows, LANES), 0)
                    row = jnp.where(j < i, row, jnp.where(j == i, 1.0, 0.0))
                row = row * root
                one = row.astype(jnp.bfloat16)
                two = (row - one.astype(jnp.float32)).astype(jnp.bfloat16)
                for piece, part in enumerate((one, one, two, two, one)):
                    weights[i, pl.ds(piece * even, rows), :] = part
                if i >= even:
                    first = root.astype(jnp.bfloat16)
                    second = (root - first.astype(jnp.float32)).astype(jnp.bfloat16)
                    j = lax.broadcasted_iota(jnp.int32, (16, LANES), 0)
                    tail = jnp.zeros((16, LANES), jnp.float32)
                    for piece, part in enumerate((first, first, second, second, first)):
                        tail = jnp.where(j == piece, part.astype(jnp.float32), tail)
                    weights[i, pl.ds(PIECES * even, 16), :] = tail.astype(jnp.bfloat16)
            row_const = halfdet[pl.ds(s, 1), :]

            def one_tile(place_at, cc):
                before = order_s[jnp.maximum(place_at - 1, 0)]
                side = lax.rem(place_at, 2)

                @pl.when(place_at >= 3)
                def _():
                    store(0, 1 - side).wait()

                flipped[...] = following[...]
                prepare(order_s[place_at + 1], following)
                conclude(before, 1 - side)
                for i in range(0, n, 2):
                    if i + 1 < n:
                        right = jnp.concatenate([weights[i], weights[i + 1]], axis=1)
                    else:
                        right = weights[i]
                    white = jnp.dot(flipped[...], right, preferred_element_type=jnp.float32)
                    square = white[:, :LANES] * white[:, :LANES]
                    if i + 1 < n:
                        square = square + white[:, LANES:] * white[:, LANES:]
                    if i:
                        acc[...] += square
                    else:
                        acc[...] = square
                done[...] = row_const - 0.5 * acc[...]

                @pl.when(place_at >= 1)
                def _():
                    store(before, 1 - side).start()

                return cc

            lax.fori_loop(start_s[slot], start_s[slot + 1], one_tile, 0)
            return c

        lax.fori_loop(base, jnp.minimum(used, base + SUB), one_slot, 0)
        return carry

    lax.fori_loop(0, (used + SUB - 1) // SUB, one_batch, 0)
    last = order_s[tiles - 1]
    side = (tiles - 1) % 2
    if tiles >= 3:
        store(0, side).wait()
    conclude(last, side)
    store(last, side).start()
    if tiles >= 2:
        store(0, 1 - side).wait()
    store(last, side).wait()


def shifted_scores(effects, se_table, se_index, covar, grid_scale, comp_grid, weights):
    n, pairs = effects.shape
    patterns = se_table.shape[0]
    tiles = pairs // TILE
    even = n // 16 * 16
    assert covar.shape == (n * n, LANES) and (n - even) * PIECES <= 16
    depth = PIECES * even + 16
    vmem = pl.BlockSpec(memory_space=pltpu.VMEM)
    smem = pl.BlockSpec(memory_space=pltpu.SMEM)
    hbm = pl.BlockSpec(memory_space=pl.ANY)
    f32 = jnp.float32
    return pl.pallas_call(
        functools.partial(main_kernel, n, tiles, patterns, grid_scale.shape[0]),
        name="shifted_scores",
        out_shape=(
            jax.ShapeDtypeStruct((LANES, pairs), f32),
            jax.ShapeDtypeStruct((2, pairs), f32),
        ),
        in_specs=[smem, smem, hbm, vmem, vmem, vmem, vmem],
        out_specs=(hbm, vmem),
        scratch_shapes=[
            pltpu.VMEM((n * n * SUB, LANES), f32),
            pltpu.VMEM((n * SUB, LANES), f32),
            pltpu.VMEM((block_edge(n) * n * SUB, LANES), f32),
            pltpu.VMEM((n * SUB, LANES), f32),
            pltpu.VMEM((SUB, LANES), f32),
            pltpu.VMEM((n * SUB, LANES), f32),
            pltpu.VMEM((n, depth, LANES), jnp.bfloat16),
            pltpu.VMEM((n, pairs), f32),
            pltpu.VMEM((TILE, depth), jnp.bfloat16),
            pltpu.VMEM((TILE, depth), jnp.bfloat16),
            pltpu.VMEM((depth, TILE), f32),
            pltpu.VMEM((TILE, LANES), f32),
            pltpu.VMEM((TILE, LANES), f32),
            pltpu.VMEM((2, LANES, TILE), f32),
            pltpu.VMEM((SUB, n), f32),
            pltpu.SemaphoreType.DMA,
            pltpu.SemaphoreType.DMA((2,)),
            pltpu.SMEM((patterns + 1,), jnp.int32),
            pltpu.SMEM((patterns + 1,), jnp.int32),
            pltpu.SMEM((patterns + 1,), jnp.int32),
            pltpu.SMEM((tiles + 1,), jnp.int32),
        ],
        compiler_params=pltpu.CompilerParams(vmem_limit_bytes=48 * 1024 * 1024),
    )(se_index, grid_scale, effects, se_table, covar, comp_grid[None], weights[None])


def exact_dot(left, right, dims):
    return lax.dot_general(left, right, (dims, ((), ())), precision=lax.Precision.HIGHEST, preferred_element_type=jnp.float32)


def finish_kernel(shifted_ref, own_ref, peaks_ref, out_ref, loglik_ref, mass_ref, partial):
    tops = [peaks_ref[c, 0:1, :] for c in range(peaks_ref.shape[0])]
    sums = [peaks_ref[c, 1:2, :] for c in range(peaks_ref.shape[0])]
    top = functools.reduce(jnp.maximum, tops)
    total = sum(s * jnp.exp(t - top) for s, t in zip(sums, tops))
    loglik = top + jnp.log(total)
    loglik_ref[...] = loglik
    value = shifted_ref[...] * jnp.exp(own_ref[0:1, :] - loglik)
    out_ref[...] = value
    chunk = value[:, :LANES]
    for c in range(1, value.shape[1] // LANES):
        chunk = chunk + value[:, c * LANES : (c + 1) * LANES]
    step = pl.program_id(0)

    @pl.when(step == 0)
    def _():
        partial[...] = chunk

    @pl.when(step > 0)
    def _():
        partial[...] += chunk

    @pl.when(step == pl.num_programs(0) - 1)
    def _():
        mass = jnp.sum(jnp.transpose(partial[...]), axis=0, keepdims=True)
        mass_ref[...] = jnp.broadcast_to(mass, mass_ref.shape)


def finish(shifted, peak, peaks, receivers):
    comps, pairs = shifted.shape
    width = min(pairs, 1024)
    return pl.pallas_call(
        finish_kernel,
        name="finish",
        grid=(pairs // width,),
        in_specs=[
            pl.BlockSpec((comps, width), lambda g: (0, g)),
            pl.BlockSpec((2, width), lambda g: (0, g)),
            pl.BlockSpec((peaks.shape[0], 2, width), lambda g: (0, 0, g)),
        ],
        out_specs=(
            pl.BlockSpec((comps, width), lambda g: (0, g)),
            pl.BlockSpec((1, width), lambda g: (0, g)),
            pl.BlockSpec((receivers, comps), lambda g: (0, 0)),
        ),
        out_shape=(
            jax.ShapeDtypeStruct((comps, pairs), jnp.float32),
            jax.ShapeDtypeStruct((1, pairs), jnp.float32),
            jax.ShapeDtypeStruct((receivers, comps), jnp.float32),
        ),
        scratch_shapes=[pltpu.VMEM((LANES, LANES), jnp.float32)],
    )(shifted, peak, peaks)


def per_device(effects, se_table, se_index, base_root, grid_scale, comp_base, comp_grid, weights):
    n, pairs = effects.shape
    comps = comp_base.shape[0]
    covariances = jnp.einsum("uij,ukj->uik", base_root, base_root, precision=lax.Precision.HIGHEST)
    covariances = covariances.reshape(covariances.shape[0], n * n)
    bases = jnp.arange(covariances.shape[0], dtype=jnp.int32)
    pick = (comp_base[None] == bases[:, None]).astype(jnp.float32)
    covar = exact_dot(covariances, pick, ((0,), (0,)))
    shifted, peak = shifted_scores(effects, se_table, se_index, covar, grid_scale, comp_grid, weights)
    peaks = lax.all_gather(peak, "comp")
    receivers = lax.axis_size("pairs")
    responsibility, loglik, mass = finish(shifted, peak, peaks, receivers)
    masses = jnp.sum(lax.all_to_all(mass, "pairs", 0, 0, tiled=True), axis=0)
    all_pairs = pairs * lax.axis_size("pairs")
    all_comps = comps * lax.axis_size("comp")
    log_weights = jnp.log((masses + 1.0) / (all_pairs + all_comps))
    return (responsibility, log_weights, loglik[0])


def solution(mesh):
    placed = (P(None, "pairs"), P(), P("pairs"), P(), P(), P("comp"), P("comp"), P("comp"))
    return jax.shard_map(
        per_device,
        mesh=mesh,
        in_specs=placed,
        out_specs=(P("comp", "pairs"), P("comp"), P("pairs")),
        check_vma=False,
    )
```

```python
import functools
import math

import jax
import jax.numpy as jnp
from jax import lax
from jax.experimental import pallas as pl
from jax.experimental.pallas import tpu as pltpu
from jax.sharding import PartitionSpec as P

TILE = 512
SUB = 8
LANES = 128
PIECES = 5


def block_edge(count):
    return max(edge for edge in range(1, 9) if count % edge == 0)


def element(index):
    return pl.ds(pl.multiple_of(index * SUB, SUB), SUB)


def eliminate(n, table, pivots, factors):
    edge = block_edge(n)
    blocks = n // edge

    def at(i, j):
        return element(i * n + j)

    def one_pivot_block(kb, carry):
        first = kb * edge
        diag = [[table[at(first + m, first + j), :] if j >= m else None for j in range(edge)] for m in range(edge)]
        lower = [[None] * edge for _ in range(edge)]
        inverse = [[None] * edge for _ in range(edge)]
        recips = []
        for m in range(edge):
            d = diag[m][m]
            recip = 1.0 / d
            recips.append(recip)
            pivots[element(first + m), :] = d
            for r in range(m + 1, edge):
                lower[r][m] = diag[m][r] * recip
            for r in range(m + 1, edge):
                for j in range(r, edge):
                    diag[r][j] = diag[r][j] - lower[r][m] * diag[m][j]
                for j in range(m):
                    inverse[r][j] = inverse[r][j] - lower[r][m] * inverse[m][j]
                inverse[r][m] = -lower[r][m]
        for r in range(edge):
            for j in range(r):
                table[at(first + r, first + j), :] = inverse[r][j]

        def column_block(jb, with_factor):
            col = jb * edge
            for j in range(edge):
                rows = [table[at(first + m, col + j), :] for m in range(edge)]
                for m in range(edge):
                    for r in range(m + 1, edge):
                        rows[r] = rows[r] - lower[r][m] * rows[m]
                for m in range(edge):
                    if m:
                        table[at(first + m, col + j), :] = rows[m]
                    if with_factor:
                        factors[element(m * n + col + j), :] = rows[m] * recips[m]

        def left(jb, c):
            column_block(jb, False)
            return c

        def right(jb, c):
            column_block(jb, True)
            return c

        lax.fori_loop(0, kb, left, 0)
        lax.fori_loop(kb + 1, blocks, right, 0)

        def row_block(ib, c):
            row = ib * edge
            start = 0
            for size in (edge - edge // 2, edge // 2):
                rows = range(start, start + size)
                start += size
                f = [[factors[element(m * n + row + i), :] for m in range(edge)] for i in rows]
                for j in range(edge):
                    totals = [f[a][j] for a in range(size)]
                    for m in range(j + 1, edge):
                        v = table[at(first + m, first + j), :]
                        totals = [totals[a] + f[a][m] * v for a in range(size)]
                    for a, i in enumerate(rows):
                        table[at(row + i, first + j), :] = -totals[a]
                for j in range(rows[0], edge):
                    live = [a for a, i in enumerate(rows) if i <= j]
                    values = [table[at(row + rows[a], row + j), :] for a in live]
                    for m in range(edge):
                        u = table[at(first + m, row + j), :]
                        values = [v - f[a][m] * u for a, v in zip(live, values)]
                    for a, v in zip(live, values):
                        table[at(row + rows[a], row + j), :] = v

            def full(index, cc):
                jb = jnp.where(index < kb, index, index - kb + ib + 1)
                col = jb * edge
                start = 0
                for size in (edge - edge // 2, edge // 2):
                    rows = range(start, start + size)
                    start += size
                    held = [[table[at(row + i, col + j), :] for j in range(edge)] for i in rows]
                    for m in range(edge):
                        f = [factors[element(m * n + row + i), :] for i in rows]
                        for j in range(edge):
                            u = table[at(first + m, col + j), :]
                            for a in range(len(f)):
                                held[a][j] = held[a][j] - f[a] * u
                    for a, i in enumerate(rows):
                        for j in range(edge):
                            table[at(row + i, col + j), :] = held[a][j]
                return cc

            lax.fori_loop(0, kb + blocks - 1 - ib, full, 0)
            return c

        lax.fori_loop(kb + 1, blocks, row_block, 0)
        return carry

    lax.fori_loop(0, blocks, one_pivot_block, 0)


def split3(value):
    one = value.astype(jnp.bfloat16)
    rest = value - one.astype(jnp.float32)
    two = rest.astype(jnp.bfloat16)
    three = (rest - two.astype(jnp.float32)).astype(jnp.bfloat16)
    return one, two, three


def main_kernel(
    n, tiles, patterns, grids,
    index_ref, grid_ref, effects_hbm, se_ref, covar_hbm, comp_grid_ref, prior_ref,
    out_hbm, peak_ref,
    table, pivots, factors, roots, halfdet, noise, weights, effects_ref, covar_ref, flipped, following, stack, acc, done, out_buf, se_rows,
    in_sem, covar_sem, out_sem,
    count_s, start_s, slot_s, order_s,
):
    even = n // 16 * 16
    edge_rows = n - even
    edge = block_edge(n)
    fetch = pltpu.make_async_copy(effects_hbm, effects_ref, in_sem)
    fetch.start()
    fetch_covar = pltpu.make_async_copy(covar_hbm, covar_ref, covar_sem)
    fetch_covar.start()

    def clear(b, c):
        count_s[b] = 0
        return c

    lax.fori_loop(0, patterns, clear, 0)

    def tally(t, c):
        b = index_ref[t]
        count_s[b] = count_s[b] + 1
        return c

    lax.fori_loop(0, tiles, tally, 0)

    def place(b, state):
        used, offset = state
        many = count_s[b]
        slot_s[used] = b
        start_s[used] = offset
        count_s[b] = offset
        return used + jnp.where(many > 0, 1, 0), offset + many

    used, _ = lax.fori_loop(0, patterns, place, (jnp.int32(0), jnp.int32(0)))
    start_s[used] = tiles

    def sort(t, c):
        b = index_ref[t]
        position = count_s[b]
        order_s[position] = t
        count_s[b] = position + 1
        return c

    lax.fori_loop(0, tiles, sort, 0)
    order_s[tiles] = 0

    weights[...] = jnp.zeros_like(weights)
    stack[...] = jnp.zeros_like(stack)
    chosen = comp_grid_ref[...]
    scale = jnp.zeros(chosen.shape, jnp.float32)
    for g in range(grids):
        scale = jnp.where(chosen == g, grid_ref[g], scale)
    scale = jnp.broadcast_to(scale * scale, (SUB, LANES))
    log_prior = jnp.log(prior_ref[...]) - 0.5 * n * math.log(2.0 * math.pi)

    fetch_covar.wait()

    def columns(t):
        return pl.ds(pl.multiple_of(t * TILE, TILE), TILE)

    def prepare(t, target):
        at = columns(t)
        data = effects_ref[pl.ds(0, even), at]
        x1, x2, x3 = split3(data)
        for piece, part in enumerate((x1, x2, x1, x2, x3)):
            stack[pl.ds(piece * even, even), :] = part.astype(jnp.float32)
        for extra in range(edge_rows):
            line = effects_ref[pl.ds(even + extra, 1), at]
            x1, x2, x3 = split3(line)
            for piece, part in enumerate((x1, x2, x1, x2, x3)):
                stack[pl.ds(PIECES * even + extra * PIECES + piece, 1), :] = part.astype(jnp.float32)
        target[...] = jnp.transpose(stack[...]).astype(jnp.bfloat16)

    def conclude(t, side):
        at = columns(t)
        scores = jnp.transpose(done[...])
        top = jnp.max(scores, axis=0, keepdims=True)
        shifted = jnp.exp(scores - top)
        out_buf[side] = shifted
        peak_ref[0:1, at] = top
        peak_ref[1:2, at] = jnp.sum(shifted, axis=0, keepdims=True)

    def store(t, side):
        return pltpu.make_async_copy(out_buf.at[side], out_hbm.at[:, columns(t)], out_sem.at[side])

    def one_batch(batch, carry):
        base = batch * SUB
        for s in range(SUB):
            b = slot_s[jnp.minimum(base + s, used - 1)]
            se_rows[pl.ds(s, 1), :] = se_ref[pl.ds(b, 1), :]
        ses = se_rows[...]
        squares = ses * ses
        for i in range(n):
            noise[pl.ds(i * SUB, SUB), :] = jnp.broadcast_to(squares[:, i : i + 1], (SUB, LANES))

        for rb in range(n // edge):
            def fill_row(i, c):
                for j in range(rb * edge, n):
                    e = i * n + j
                    table[element(e), :] = covar_ref[pl.ds(e, SUB, stride=0), :] * scale
                d = element(i * n + i)
                table[d, :] = table[d, :] + noise[element(i), :]
                return c

            lax.fori_loop(rb * edge, (rb + 1) * edge, fill_row, 0)
        eliminate(n, table, pivots, factors)
        logs = jnp.zeros((SUB, LANES), jnp.float32)
        for i in range(n):
            d = pivots[pl.ds(i * SUB, SUB), :]
            roots[pl.ds(i * SUB, SUB), :] = lax.rsqrt(d)
            logs = logs + jnp.log(d)
        halfdet[...] = log_prior - 0.5 * logs

        @pl.when(batch == 0)
        def _():
            fetch.wait()
            prepare(order_s[0], following)

        def one_slot(slot, c):
            s = slot - base
            for i in range(n):
                groups = min(i // 16 + 1, even // 16)
                rows = groups * 16
                root = roots[pl.ds(i * SUB + s, SUB, stride=0), :][0:1, :]
                row = table[pl.ds(i * n * SUB + s, rows, stride=SUB), :]
                if i < even:
                    j = lax.broadcasted_iota(jnp.int32, (rows, LANES), 0)
                    row = jnp.where(j < i, row, jnp.where(j == i, 1.0, 0.0))
                row = row * root
                one = row.astype(jnp.bfloat16)
                two = (row - one.astype(jnp.float32)).astype(jnp.bfloat16)
                for piece, part in enumerate((one, one, two, two, one)):
                    weights[i, pl.ds(piece * even, rows), :] = part
                if i >= even:
                    first = root.astype(jnp.bfloat16)
                    second = (root - first.astype(jnp.float32)).astype(jnp.bfloat16)
                    j = lax.broadcasted_iota(jnp.int32, (16, LANES), 0)
                    tail = jnp.zeros((16, LANES), jnp.float32)
                    for piece, part in enumerate((first, first, second, second, first)):
                        tail = jnp.where(j == piece, part.astype(jnp.float32), tail)
                    weights[i, pl.ds(PIECES * even, 16), :] = tail.astype(jnp.bfloat16)
            row_const = halfdet[pl.ds(s, 1), :]

            def one_tile(place_at, cc):
                before = order_s[jnp.maximum(place_at - 1, 0)]
                side = lax.rem(place_at, 2)

                @pl.when(place_at >= 3)
                def _():
                    store(0, 1 - side).wait()

                flipped[...] = following[...]
                prepare(order_s[place_at + 1], following)
                conclude(before, 1 - side)
                for i in range(0, n, 2):
                    if i + 1 < n:
                        right = jnp.concatenate([weights[i], weights[i + 1]], axis=1)
                    else:
                        right = weights[i]
                    white = jnp.dot(flipped[...], right, preferred_element_type=jnp.float32)
                    square = white[:, :LANES] * white[:, :LANES]
                    if i + 1 < n:
                        square = square + white[:, LANES:] * white[:, LANES:]
                    if i:
                        acc[...] += square
                    else:
                        acc[...] = square
                done[...] = row_const - 0.5 * acc[...]

                @pl.when(place_at >= 1)
                def _():
                    store(before, 1 - side).start()

                return cc

            lax.fori_loop(start_s[slot], start_s[slot + 1], one_tile, 0)
            return c

        lax.fori_loop(base, jnp.minimum(used, base + SUB), one_slot, 0)
        return carry

    lax.fori_loop(0, (used + SUB - 1) // SUB, one_batch, 0)
    last = order_s[tiles - 1]
    side = (tiles - 1) % 2
    if tiles >= 3:
        store(0, side).wait()
    conclude(last, side)
    store(last, side).start()
    if tiles >= 2:
        store(0, 1 - side).wait()
    store(last, side).wait()


def shifted_scores(effects, se_table, se_index, covar, grid_scale, comp_grid, weights):
    n, pairs = effects.shape
    patterns = se_table.shape[0]
    tiles = pairs // TILE
    even = n // 16 * 16
    assert covar.shape == (n * n, LANES) and (n - even) * PIECES <= 16
    depth = PIECES * even + 16
    vmem = pl.BlockSpec(memory_space=pltpu.VMEM)
    smem = pl.BlockSpec(memory_space=pltpu.SMEM)
    hbm = pl.BlockSpec(memory_space=pl.ANY)
    f32 = jnp.float32
    return pl.pallas_call(
        functools.partial(main_kernel, n, tiles, patterns, grid_scale.shape[0]),
        name="shifted_scores",
        out_shape=(
            jax.ShapeDtypeStruct((LANES, pairs), f32),
            jax.ShapeDtypeStruct((2, pairs), f32),
        ),
        in_specs=[smem, smem, hbm, vmem, hbm, vmem, vmem],
        out_specs=(hbm, vmem),
        scratch_shapes=[
            pltpu.VMEM((n * n * SUB, LANES), f32),
            pltpu.VMEM((n * SUB, LANES), f32),
            pltpu.VMEM((block_edge(n) * n * SUB, LANES), f32),
            pltpu.VMEM((n * SUB, LANES), f32),
            pltpu.VMEM((SUB, LANES), f32),
            pltpu.VMEM((n * SUB, LANES), f32),
            pltpu.VMEM((n, depth, LANES), jnp.bfloat16),
            pltpu.VMEM((n, pairs), f32),
            pltpu.VMEM((n * n, LANES), f32),
            pltpu.VMEM((TILE, depth), jnp.bfloat16),
            pltpu.VMEM((TILE, depth), jnp.bfloat16),
            pltpu.VMEM((depth, TILE), f32),
            pltpu.VMEM((TILE, LANES), f32),
            pltpu.VMEM((TILE, LANES), f32),
            pltpu.VMEM((2, LANES, TILE), f32),
            pltpu.VMEM((SUB, n), f32),
            pltpu.SemaphoreType.DMA,
            pltpu.SemaphoreType.DMA,
            pltpu.SemaphoreType.DMA((2,)),
            pltpu.SMEM((patterns + 1,), jnp.int32),
            pltpu.SMEM((patterns + 1,), jnp.int32),
            pltpu.SMEM((patterns + 1,), jnp.int32),
            pltpu.SMEM((tiles + 1,), jnp.int32),
        ],
        compiler_params=pltpu.CompilerParams(vmem_limit_bytes=26 * 1024 * 1024),
    )(se_index, grid_scale, effects, se_table, covar, comp_grid[None], weights[None])


def exact_dot(left, right, dims):
    return lax.dot_general(left, right, (dims, ((), ())), precision=lax.Precision.HIGHEST, preferred_element_type=jnp.float32)


def finish_kernel(width, shifted_ref, own_ref, peaks_ref, out_hbm, loglik_ref, mass_ref, buffer, sems):
    pairs = shifted_ref.shape[1]
    steps = pairs // width
    copies = []
    partial = None
    for step in range(steps):
        at = pl.ds(step * width, width)
        tops = [peaks_ref[c, 0:1, at] for c in range(peaks_ref.shape[0])]
        sums = [peaks_ref[c, 1:2, at] for c in range(peaks_ref.shape[0])]
        top = functools.reduce(jnp.maximum, tops)
        total = sum(s * jnp.exp(t - top) for s, t in zip(sums, tops))
        loglik = top + jnp.log(total)
        loglik_ref[:, at] = loglik
        factor = jnp.exp(own_ref[0:1, at] - loglik)
        for c in range(width // LANES):
            lanes = pl.ds(step * width + c * LANES, LANES)
            value = shifted_ref[:, lanes] * factor[:, c * LANES : (c + 1) * LANES]
            buffer[:, lanes] = value
            partial = value if partial is None else partial + value
        copy = pltpu.make_async_copy(buffer.at[:, at], out_hbm.at[:, at], sems.at[step])
        copy.start()
        copies.append(copy)
    mass = jnp.sum(jnp.transpose(partial), axis=0, keepdims=True)
    mass_ref[...] = jnp.broadcast_to(mass, mass_ref.shape)
    for copy in copies:
        copy.wait()


def finish(shifted, peak, peaks, receivers):
    comps, pairs = shifted.shape
    width = min(pairs, 1024)
    vmem = pl.BlockSpec(memory_space=pltpu.VMEM)
    return pl.pallas_call(
        functools.partial(finish_kernel, width),
        name="finish",
        in_specs=[vmem, vmem, vmem],
        out_specs=(pl.BlockSpec(memory_space=pl.ANY), vmem, vmem),
        out_shape=(
            jax.ShapeDtypeStruct((comps, pairs), jnp.float32),
            jax.ShapeDtypeStruct((1, pairs), jnp.float32),
            jax.ShapeDtypeStruct((receivers, comps), jnp.float32),
        ),
        scratch_shapes=[pltpu.VMEM((comps, pairs), jnp.float32), pltpu.SemaphoreType.DMA((pairs // width,))],
        compiler_params=pltpu.CompilerParams(vmem_limit_bytes=12 * 1024 * 1024),
    )(shifted, peak, peaks)


def per_device(effects, se_table, se_index, base_root, grid_scale, comp_base, comp_grid, weights):
    n, pairs = effects.shape
    comps = comp_base.shape[0]
    covariances = jnp.einsum("uij,ukj->uik", base_root, base_root, precision=lax.Precision.HIGHEST)
    covariances = covariances.reshape(covariances.shape[0], n * n)
    bases = jnp.arange(covariances.shape[0], dtype=jnp.int32)
    pick = (comp_base[None] == bases[:, None]).astype(jnp.float32)
    covar = exact_dot(covariances, pick, ((0,), (0,)))
    shifted, peak = shifted_scores(effects, se_table, se_index, covar, grid_scale, comp_grid, weights)
    peaks = lax.all_gather(peak, "comp")
    receivers = lax.axis_size("pairs")
    responsibility, loglik, mass = finish(shifted, peak, peaks, receivers)
    masses = jnp.sum(lax.all_to_all(mass, "pairs", 0, 0, tiled=True), axis=0)
    all_pairs = pairs * lax.axis_size("pairs")
    all_comps = comps * lax.axis_size("comp")
    log_weights = jnp.log((masses + 1.0) / (all_pairs + all_comps))
    return (responsibility, log_weights, loglik[0])


def solution(mesh):
    placed = (P(None, "pairs"), P(), P("pairs"), P(), P(), P("comp"), P("comp"), P("comp"))
    return jax.shard_map(
        per_device,
        mesh=mesh,
        in_specs=placed,
        out_specs=(P("comp", "pairs"), P("comp"), P("pairs")),
        check_vma=False,
    )
```

```python
import functools
import math

import jax
import jax.numpy as jnp
import numpy as np
from jax import lax
from jax.experimental import pallas as pl
from jax.experimental.pallas import tpu as pltpu
from jax.sharding import PartitionSpec as P

TILE = 512
SUB = 8
LANES = 128
PIECES = 5
GROUP = 5


def block_edge(count):
    return max(edge for edge in range(1, 9) if count % edge == 0)


def element(index):
    return pl.ds(pl.multiple_of(index * SUB, SUB), SUB)


def update_plan(blocks, group):
    lists = []
    for kb in range(blocks):
        pairs = [(ib, jb) for ib in range(kb + 1, blocks) for jb in list(range(kb)) + list(range(ib + 1, blocks))]
        while len(pairs) % group:
            pairs.append((blocks, 0))
        lists.append(pairs)
    flat = [pair for pairs in lists for pair in pairs]
    starts = np.cumsum([0] + [len(pairs) for pairs in lists])
    ends = [starts[kb] + sum(ib < blocks for ib, _ in pairs) for kb, pairs in enumerate(lists)]
    return tuple(np.array(a, np.int32) for a in ([p[0] for p in flat], [p[1] for p in flat], starts, ends))


def elimination(n, table, pivots, factors):
    edge = block_edge(n)
    blocks = n // edge

    def at(q, i, j):
        return element(q * (n + edge) * n + i * n + j)

    def pivot_stage(q, kb):
        first = kb * edge
        diag = [[table[at(q, first + m, first + j), :] if j >= m else None for j in range(edge)] for m in range(edge)]
        lower = [[None] * edge for _ in range(edge)]
        inverse = [[None] * edge for _ in range(edge)]
        recips = []
        for m in range(edge):
            d = diag[m][m]
            recip = 1.0 / d
            recips.append(recip)
            pivots[element(first + m), :] = d
            for r in range(m + 1, edge):
                lower[r][m] = diag[m][r] * recip
            for r in range(m + 1, edge):
                for j in range(r, edge):
                    diag[r][j] = diag[r][j] - lower[r][m] * diag[m][j]
                for j in range(m):
                    inverse[r][j] = inverse[r][j] - lower[r][m] * inverse[m][j]
                inverse[r][m] = -lower[r][m]
        for r in range(edge):
            for j in range(r):
                table[at(q, first + r, first + j), :] = inverse[r][j]

        def column_block(jb, with_factor):
            col = jb * edge
            for j in range(edge):
                rows = [table[at(q, first + m, col + j), :] for m in range(edge)]
                for m in range(edge):
                    for r in range(m + 1, edge):
                        rows[r] = rows[r] - lower[r][m] * rows[m]
                for m in range(edge):
                    if m:
                        table[at(q, first + m, col + j), :] = rows[m]
                    if with_factor:
                        factors[element(m * n + col + j), :] = rows[m] * recips[m]

        def left(jb, c):
            column_block(jb, False)
            return c

        def right(jb, c):
            column_block(jb, True)
            return c

        lax.fori_loop(0, kb, left, 0)
        lax.fori_loop(kb + 1, blocks, right, 0)

        def row_block(ib, c):
            row = ib * edge
            start = 0
            for size in (edge - edge // 2, edge // 2):
                rows = range(start, start + size)
                start += size
                f = [[factors[element(m * n + row + i), :] for m in range(edge)] for i in rows]
                for j in range(edge):
                    totals = [f[a][j] for a in range(size)]
                    for m in range(j + 1, edge):
                        v = table[at(q, first + m, first + j), :]
                        totals = [totals[a] + f[a][m] * v for a in range(size)]
                    for a, i in enumerate(rows):
                        table[at(q, row + i, first + j), :] = -totals[a]
                for j in range(rows[0], edge):
                    live = [a for a, i in enumerate(rows) if i <= j]
                    values = [table[at(q, row + rows[a], row + j), :] for a in live]
                    for m in range(edge):
                        u = table[at(q, first + m, row + j), :]
                        values = [v - f[a][m] * u for a, v in zip(live, values)]
                    for a, v in zip(live, values):
                        table[at(q, row + rows[a], row + j), :] = v
            return c

        lax.fori_loop(kb + 1, blocks, row_block, 0)

    def update(q, kb, ib, jb):
        first, row, col = kb * edge, ib * edge, jb * edge
        start = 0
        for size in (edge - edge // 2, edge // 2):
            rows = range(start, start + size)
            start += size
            held = [[table[at(q, row + i, col + j), :] for j in range(edge)] for i in rows]
            for m in range(edge):
                f = [factors[element(m * n + row + i), :] for i in rows]
                for j in range(edge):
                    u = table[at(q, first + m, col + j), :]
                    for a in range(len(f)):
                        held[a][j] = held[a][j] - f[a] * u
            for a, i in enumerate(rows):
                for j in range(edge):
                    table[at(q, row + i, col + j), :] = held[a][j]

    return at, pivot_stage, update


def split3(value):
    one = value.astype(jnp.bfloat16)
    rest = value - one.astype(jnp.float32)
    two = rest.astype(jnp.bfloat16)
    three = (rest - two.astype(jnp.float32)).astype(jnp.bfloat16)
    return one, two, three


def main_kernel(
    n, tiles, patterns, grids,
    index_ref, grid_ref, plan_row, plan_col, plan_start, plan_end, effects_hbm, se_ref, covar_hbm, comp_grid_ref, prior_ref,
    out_hbm, peak_ref,
    table, pivots, factors, roots, halfdet, noise, weights, effects_ref, covar_ref, flipped, following, stack, acc, done, out_buf, se_rows,
    in_sem, covar_sem, out_sem,
    count_s, start_s, slot_s, order_s, state_s,
):
    even = n // 16 * 16
    edge_rows = n - even
    edge = block_edge(n)
    blocks = n // edge
    at_block, pivot_stage, update = elimination(n, table, pivots, factors)
    fetch = pltpu.make_async_copy(effects_hbm, effects_ref, in_sem)
    fetch.start()
    fetch_covar = pltpu.make_async_copy(covar_hbm, covar_ref, covar_sem)
    fetch_covar.start()

    def clear(b, c):
        count_s[b] = 0
        return c

    lax.fori_loop(0, patterns, clear, 0)

    def tally(t, c):
        b = index_ref[t]
        count_s[b] = count_s[b] + 1
        return c

    lax.fori_loop(0, tiles, tally, 0)

    def place(b, state):
        used, offset = state
        many = count_s[b]
        slot_s[used] = b
        start_s[used] = offset
        count_s[b] = offset
        return used + jnp.where(many > 0, 1, 0), offset + many

    used, _ = lax.fori_loop(0, patterns, place, (jnp.int32(0), jnp.int32(0)))
    start_s[used] = tiles

    def sort(t, c):
        b = index_ref[t]
        position = count_s[b]
        order_s[position] = t
        count_s[b] = position + 1
        return c

    lax.fori_loop(0, tiles, sort, 0)
    order_s[tiles] = 0

    weights[...] = jnp.zeros_like(weights)
    stack[...] = jnp.zeros_like(stack)
    chosen = comp_grid_ref[...]
    scale = jnp.zeros(chosen.shape, jnp.float32)
    for g in range(grids):
        scale = jnp.where(chosen == g, grid_ref[g], scale)
    scale = jnp.broadcast_to(scale * scale, (SUB, LANES))
    log_prior = jnp.log(prior_ref[...]) - 0.5 * n * math.log(2.0 * math.pi)

    fetch_covar.wait()

    def columns(t):
        return pl.ds(pl.multiple_of(t * TILE, TILE), TILE)

    def prepare(t, target):
        at = columns(t)
        data = effects_ref[pl.ds(0, even), at]
        x1, x2, x3 = split3(data)
        for piece, part in enumerate((x1, x2, x1, x2, x3)):
            stack[pl.ds(piece * even, even), :] = part.astype(jnp.float32)
        for extra in range(edge_rows):
            line = effects_ref[pl.ds(even + extra, 1), at]
            x1, x2, x3 = split3(line)
            for piece, part in enumerate((x1, x2, x1, x2, x3)):
                stack[pl.ds(PIECES * even + extra * PIECES + piece, 1), :] = part.astype(jnp.float32)
        target[...] = jnp.transpose(stack[...]).astype(jnp.bfloat16)

    def conclude(t, side):
        at = columns(t)
        scores = jnp.transpose(done[...])
        top = jnp.max(scores, axis=0, keepdims=True)
        shifted = jnp.exp(scores - top)
        out_buf[side] = shifted
        peak_ref[0:1, at] = top
        peak_ref[1:2, at] = jnp.sum(shifted, axis=0, keepdims=True)

    def store(t, side):
        return pltpu.make_async_copy(out_buf.at[side], out_hbm.at[:, columns(t)], out_sem.at[side])

    def fill(batch):
        base = batch * SUB
        q = lax.rem(batch, 2)
        for s in range(SUB):
            b = slot_s[jnp.minimum(base + s, used - 1)]
            se_rows[pl.ds(s, 1), :] = se_ref[pl.ds(b, 1), :]
        ses = se_rows[...]
        squares = ses * ses
        for i in range(n):
            noise[pl.ds(i * SUB, SUB), :] = jnp.broadcast_to(squares[:, i : i + 1], (SUB, LANES))

        for rb in range(blocks):
            def fill_row(i, c):
                for j in range(rb * edge, n):
                    table[at_block(q, i, j), :] = covar_ref[pl.ds(i * n + j, SUB, stride=0), :] * scale
                d = at_block(q, i, i)
                table[d, :] = table[d, :] + noise[element(i), :]
                return c

            lax.fori_loop(rb * edge, (rb + 1) * edge, fill_row, 0)

    def advance(q):
        kb = state_s[0]

        @pl.when(state_s[1] >= plan_start[kb + 1])
        def _():
            state_s[0] = kb + 1

            @pl.when(kb + 1 < blocks)
            def _():
                pivot_stage(q, kb + 1)

    def begin(q):
        state_s[0] = 0
        state_s[1] = 0
        pivot_stage(q, 0)

    def drain(q):
        def one_block(kb, c):
            position = state_s[1]

            def one(p, cc):
                update(q, kb, plan_row[p], plan_col[p])
                return cc

            lax.fori_loop(position, plan_end[kb], one, 0)
            state_s[1] = plan_start[kb + 1]

            @pl.when(kb + 1 < blocks)
            def _():
                pivot_stage(q, kb + 1)

            return c

        lax.fori_loop(state_s[0], blocks, one_block, 0)

    def one_batch(batch, carry):
        base = batch * SUB
        q = lax.rem(batch, 2)
        more = base + SUB < used

        @pl.when(batch == 0)
        def _():
            fill(batch)
            begin(q)

        drain(q)
        state_s[0] = blocks
        logs = jnp.zeros((SUB, LANES), jnp.float32)
        for i in range(n):
            d = pivots[pl.ds(i * SUB, SUB), :]
            roots[pl.ds(i * SUB, SUB), :] = lax.rsqrt(d)
            logs = logs + jnp.log(d)
        halfdet[...] = log_prior - 0.5 * logs

        @pl.when(batch == 0)
        def _():
            fetch.wait()
            prepare(order_s[0], following)

        @pl.when(more)
        def _():
            fill(batch + 1)
            begin(1 - q)

        def one_slot(slot, c):
            s = slot - base
            for i in range(n):
                groups = min(i // 16 + 1, even // 16)
                rows = groups * 16
                root = roots[pl.ds(i * SUB + s, SUB, stride=0), :][0:1, :]
                row = table[pl.ds(q * (n + edge) * n * SUB + i * n * SUB + s, rows, stride=SUB), :]
                if i < even:
                    j = lax.broadcasted_iota(jnp.int32, (rows, LANES), 0)
                    row = jnp.where(j < i, row, jnp.where(j == i, 1.0, 0.0))
                row = row * root
                one = row.astype(jnp.bfloat16)
                two = (row - one.astype(jnp.float32)).astype(jnp.bfloat16)
                for piece, part in enumerate((one, one, two, two, one)):
                    weights[i, pl.ds(piece * even, rows), :] = part
                if i >= even:
                    first = root.astype(jnp.bfloat16)
                    second = (root - first.astype(jnp.float32)).astype(jnp.bfloat16)
                    j = lax.broadcasted_iota(jnp.int32, (16, LANES), 0)
                    tail = jnp.zeros((16, LANES), jnp.float32)
                    for piece, part in enumerate((first, first, second, second, first)):
                        tail = jnp.where(j == piece, part.astype(jnp.float32), tail)
                    weights[i, pl.ds(PIECES * even, 16), :] = tail.astype(jnp.bfloat16)
            row_const = halfdet[pl.ds(s, 1), :]

            def one_tile(place_at, cc):
                before = order_s[jnp.maximum(place_at - 1, 0)]
                side = lax.rem(place_at, 2)

                @pl.when(place_at >= 3)
                def _():
                    store(0, 1 - side).wait()

                def body(beside):
                    flipped[...] = following[...]
                    prepare(order_s[place_at + 1], following)
                    conclude(before, 1 - side)
                    for i in range(0, n, 2):
                        if i + 1 < n:
                            right = jnp.concatenate([weights[i], weights[i + 1]], axis=1)
                        else:
                            right = weights[i]
                        white = jnp.dot(flipped[...], right, preferred_element_type=jnp.float32)
                        square = white[:, :LANES] * white[:, :LANES]
                        if i + 1 < n:
                            square = square + white[:, LANES:] * white[:, LANES:]
                        if i:
                            acc[...] += square
                        else:
                            acc[...] = square
                        if beside is not None and i % 10 == 2 and i // 10 < GROUP:
                            beside(i // 10)
                    done[...] = row_const - 0.5 * acc[...]

                kb = state_s[0]
                position = state_s[1]
                working = kb < blocks

                @pl.when(working)
                def _():
                    body(lambda g: update(1 - q, kb, plan_row[position + g], plan_col[position + g]))
                    state_s[1] = position + GROUP
                    advance(1 - q)

                @pl.when(jnp.logical_not(working))
                def _():
                    body(None)

                @pl.when(place_at >= 1)
                def _():
                    store(before, 1 - side).start()

                return cc

            lax.fori_loop(start_s[slot], start_s[slot + 1], one_tile, 0)
            return c

        lax.fori_loop(base, jnp.minimum(used, base + SUB), one_slot, 0)
        return carry

    lax.fori_loop(0, (used + SUB - 1) // SUB, one_batch, 0)
    last = order_s[tiles - 1]
    side = (tiles - 1) % 2
    if tiles >= 3:
        store(0, side).wait()
    conclude(last, side)
    store(last, side).start()
    if tiles >= 2:
        store(0, 1 - side).wait()
    store(last, side).wait()


def shifted_scores(effects, se_table, se_index, covar, grid_scale, comp_grid, weights):
    n, pairs = effects.shape
    patterns = se_table.shape[0]
    tiles = pairs // TILE
    even = n // 16 * 16
    assert covar.shape == (n * n, LANES) and (n - even) * PIECES <= 16
    depth = PIECES * even + 16
    edge = block_edge(n)
    plan = update_plan(n // edge, GROUP)
    vmem = pl.BlockSpec(memory_space=pltpu.VMEM)
    smem = pl.BlockSpec(memory_space=pltpu.SMEM)
    hbm = pl.BlockSpec(memory_space=pl.ANY)
    f32 = jnp.float32
    return pl.pallas_call(
        functools.partial(main_kernel, n, tiles, patterns, grid_scale.shape[0]),
        name="shifted_scores",
        out_shape=(
            jax.ShapeDtypeStruct((LANES, pairs), f32),
            jax.ShapeDtypeStruct((2, pairs), f32),
        ),
        in_specs=[smem] * 6 + [hbm, vmem, hbm, vmem, vmem],
        out_specs=(hbm, vmem),
        scratch_shapes=[
            pltpu.VMEM((2 * (n + edge) * n * SUB, LANES), f32),
            pltpu.VMEM((n * SUB, LANES), f32),
            pltpu.VMEM(((edge * n + edge) * SUB, LANES), f32),
            pltpu.VMEM((n * SUB, LANES), f32),
            pltpu.VMEM((SUB, LANES), f32),
            pltpu.VMEM((n * SUB, LANES), f32),
            pltpu.VMEM((n, depth, LANES), jnp.bfloat16),
            pltpu.VMEM((n, pairs), f32),
            pltpu.VMEM((n * n, LANES), f32),
            pltpu.VMEM((TILE, depth), jnp.bfloat16),
            pltpu.VMEM((TILE, depth), jnp.bfloat16),
            pltpu.VMEM((depth, TILE), f32),
            pltpu.VMEM((TILE, LANES), f32),
            pltpu.VMEM((TILE, LANES), f32),
            pltpu.VMEM((2, LANES, TILE), f32),
            pltpu.VMEM((SUB, n), f32),
            pltpu.SemaphoreType.DMA,
            pltpu.SemaphoreType.DMA,
            pltpu.SemaphoreType.DMA((2,)),
            pltpu.SMEM((patterns + 1,), jnp.int32),
            pltpu.SMEM((patterns + 1,), jnp.int32),
            pltpu.SMEM((patterns + 1,), jnp.int32),
            pltpu.SMEM((tiles + 1,), jnp.int32),
            pltpu.SMEM((2,), jnp.int32),
        ],
        compiler_params=pltpu.CompilerParams(vmem_limit_bytes=40 * 1024 * 1024),
    )(se_index, grid_scale, *plan, effects, se_table, covar, comp_grid[None], weights[None])


def exact_dot(left, right, dims):
    return lax.dot_general(left, right, (dims, ((), ())), precision=lax.Precision.HIGHEST, preferred_element_type=jnp.float32)


def finish_kernel(width, shifted_ref, own_ref, peaks_ref, out_hbm, loglik_ref, mass_ref, buffer, sems):
    pairs = shifted_ref.shape[1]
    steps = pairs // width
    copies = []
    partial = None
    for step in range(steps):
        at = pl.ds(step * width, width)
        tops = [peaks_ref[c, 0:1, at] for c in range(peaks_ref.shape[0])]
        sums = [peaks_ref[c, 1:2, at] for c in range(peaks_ref.shape[0])]
        top = functools.reduce(jnp.maximum, tops)
        total = sum(s * jnp.exp(t - top) for s, t in zip(sums, tops))
        loglik = top + jnp.log(total)
        loglik_ref[:, at] = loglik
        factor = jnp.exp(own_ref[0:1, at] - loglik)
        for c in range(width // LANES):
            lanes = pl.ds(step * width + c * LANES, LANES)
            value = shifted_ref[:, lanes] * factor[:, c * LANES : (c + 1) * LANES]
            buffer[:, lanes] = value
            partial = value if partial is None else partial + value
        copy = pltpu.make_async_copy(buffer.at[:, at], out_hbm.at[:, at], sems.at[step])
        copy.start()
        copies.append(copy)
    mass = jnp.sum(jnp.transpose(partial), axis=0, keepdims=True)
    mass_ref[...] = jnp.broadcast_to(mass, mass_ref.shape)
    for copy in copies:
        copy.wait()


def finish(shifted, peak, peaks, receivers):
    comps, pairs = shifted.shape
    width = min(pairs, 1024)
    vmem = pl.BlockSpec(memory_space=pltpu.VMEM)
    return pl.pallas_call(
        functools.partial(finish_kernel, width),
        name="finish",
        in_specs=[vmem, vmem, vmem],
        out_specs=(pl.BlockSpec(memory_space=pl.ANY), vmem, vmem),
        out_shape=(
            jax.ShapeDtypeStruct((comps, pairs), jnp.float32),
            jax.ShapeDtypeStruct((1, pairs), jnp.float32),
            jax.ShapeDtypeStruct((receivers, comps), jnp.float32),
        ),
        scratch_shapes=[pltpu.VMEM((comps, pairs), jnp.float32), pltpu.SemaphoreType.DMA((pairs // width,))],
        compiler_params=pltpu.CompilerParams(vmem_limit_bytes=12 * 1024 * 1024),
    )(shifted, peak, peaks)


def per_device(effects, se_table, se_index, base_root, grid_scale, comp_base, comp_grid, weights):
    n, pairs = effects.shape
    comps = comp_base.shape[0]
    covariances = jnp.einsum("uij,ukj->uik", base_root, base_root, precision=lax.Precision.HIGHEST)
    covariances = covariances.reshape(covariances.shape[0], n * n)
    bases = jnp.arange(covariances.shape[0], dtype=jnp.int32)
    pick = (comp_base[None] == bases[:, None]).astype(jnp.float32)
    covar = exact_dot(covariances, pick, ((0,), (0,)))
    shifted, peak = shifted_scores(effects, se_table, se_index, covar, grid_scale, comp_grid, weights)
    peaks = lax.all_gather(peak, "comp")
    receivers = lax.axis_size("pairs")
    responsibility, loglik, mass = finish(shifted, peak, peaks, receivers)
    masses = jnp.sum(lax.all_to_all(mass, "pairs", 0, 0, tiled=True), axis=0)
    all_pairs = pairs * lax.axis_size("pairs")
    all_comps = comps * lax.axis_size("comp")
    log_weights = jnp.log((masses + 1.0) / (all_pairs + all_comps))
    return (responsibility, log_weights, loglik[0])


def solution(mesh):
    placed = (P(None, "pairs"), P(), P("pairs"), P(), P(), P("comp"), P("comp"), P("comp"))
    return jax.shard_map(
        per_device,
        mesh=mesh,
        in_specs=placed,
        out_specs=(P("comp", "pairs"), P("comp"), P("pairs")),
        check_vma=False,
    )
```

```python
import functools
import math

import jax
import jax.numpy as jnp
import numpy as np
from jax import lax
from jax.experimental import pallas as pl
from jax.experimental.pallas import tpu as pltpu
from jax.sharding import PartitionSpec as P

TILE = 512
SUB = 8
LANES = 128
PIECES = 5
GROUP = 5
ROWS = 3


def block_edge(count):
    return max(edge for edge in range(1, 9) if count % edge == 0)


def element(index):
    return pl.ds(pl.multiple_of(index * SUB, SUB), SUB)


def update_plan(blocks, group):
    lists = []
    for kb in range(blocks):
        pairs = [(ib, jb) for ib in range(kb + 1, blocks) for jb in list(range(kb)) + list(range(ib + 1, blocks))]
        while len(pairs) % group:
            pairs.append((blocks, 0))
        lists.append(pairs)
    flat = [pair for pairs in lists for pair in pairs]
    starts = np.cumsum([0] + [len(pairs) for pairs in lists])
    ends = [starts[kb] + sum(ib < blocks for ib, _ in pairs) for kb, pairs in enumerate(lists)]
    return tuple(np.array(a, np.int32) for a in ([p[0] for p in flat], [p[1] for p in flat], starts, ends))


def elimination(n, table, pivots, factors):
    edge = block_edge(n)
    blocks = n // edge

    def at(q, i, j):
        return element(q * (n + edge) * n + i * n + j)

    def pivot_stage(q, kb):
        first = kb * edge
        diag = [[table[at(q, first + m, first + j), :] if j >= m else None for j in range(edge)] for m in range(edge)]
        lower = [[None] * edge for _ in range(edge)]
        inverse = [[None] * edge for _ in range(edge)]
        recips = []
        for m in range(edge):
            d = diag[m][m]
            recip = 1.0 / d
            recips.append(recip)
            pivots[element(first + m), :] = d
            for r in range(m + 1, edge):
                lower[r][m] = diag[m][r] * recip
            for r in range(m + 1, edge):
                for j in range(r, edge):
                    diag[r][j] = diag[r][j] - lower[r][m] * diag[m][j]
                for j in range(m):
                    inverse[r][j] = inverse[r][j] - lower[r][m] * inverse[m][j]
                inverse[r][m] = -lower[r][m]
        for r in range(edge):
            for j in range(r):
                table[at(q, first + r, first + j), :] = inverse[r][j]

        def column_block(jb, with_factor):
            col = jb * edge
            for j in range(edge):
                rows = [table[at(q, first + m, col + j), :] for m in range(edge)]
                for m in range(edge):
                    for r in range(m + 1, edge):
                        rows[r] = rows[r] - lower[r][m] * rows[m]
                for m in range(edge):
                    if m:
                        table[at(q, first + m, col + j), :] = rows[m]
                    if with_factor:
                        factors[element(m * n + col + j), :] = rows[m] * recips[m]

        def left(jb, c):
            column_block(jb, False)
            return c

        def right(jb, c):
            column_block(jb, True)
            return c

        lax.fori_loop(0, kb, left, 0)
        lax.fori_loop(kb + 1, blocks, right, 0)

        def row_block(ib, c):
            row = ib * edge
            for start in range(0, edge, ROWS):
                rows = range(start, min(start + ROWS, edge))
                size = len(rows)
                f = [[factors[element(m * n + row + i), :] for m in range(edge)] for i in rows]
                totals = [list(line) for line in f]
                for m in range(1, edge):
                    for j in range(m):
                        v = table[at(q, first + m, first + j), :]
                        for a in range(size):
                            totals[a][j] = totals[a][j] + f[a][m] * v
                values = {}
                for j in range(rows[0], edge):
                    live = [a for a, i in enumerate(rows) if i <= j]
                    for a in live:
                        values[a, j] = table[at(q, row + rows[a], row + j), :]
                    for m in range(edge):
                        u = table[at(q, first + m, row + j), :]
                        for a in live:
                            values[a, j] = values[a, j] - f[a][m] * u
                for a, i in enumerate(rows):
                    for j in range(edge):
                        table[at(q, row + i, first + j), :] = -totals[a][j]
                for (a, j), v in values.items():
                    table[at(q, row + rows[a], row + j), :] = v

            return c

        lax.fori_loop(kb + 1, blocks, row_block, 0)

    def update(q, kb, ib, jb):
        first, row, col = kb * edge, ib * edge, jb * edge
        start = 0
        for size in (edge - edge // 2, edge // 2):
            rows = range(start, start + size)
            start += size
            held = [[table[at(q, row + i, col + j), :] for j in range(edge)] for i in rows]
            for m in range(edge):
                f = [factors[element(m * n + row + i), :] for i in rows]
                for j in range(edge):
                    u = table[at(q, first + m, col + j), :]
                    for a in range(len(f)):
                        held[a][j] = held[a][j] - f[a] * u
            for a, i in enumerate(rows):
                for j in range(edge):
                    table[at(q, row + i, col + j), :] = held[a][j]

    return at, pivot_stage, update


def split3(value):
    one = value.astype(jnp.bfloat16)
    rest = value - one.astype(jnp.float32)
    two = rest.astype(jnp.bfloat16)
    three = (rest - two.astype(jnp.float32)).astype(jnp.bfloat16)
    return one, two, three


def main_kernel(
    n, tiles, patterns, grids,
    index_ref, grid_ref, plan_row, plan_col, plan_start, plan_end, effects_hbm, se_ref, covar_hbm, comp_grid_ref, prior_ref,
    out_hbm, peak_ref,
    table, pivots, factors, roots, halfdet, noise, weights, effects_ref, covar_ref, flipped, following, stack, acc, done, out_buf, se_rows,
    in_sem, covar_sem, out_sem,
    count_s, start_s, slot_s, order_s, state_s,
):
    even = n // 16 * 16
    edge_rows = n - even
    edge = block_edge(n)
    blocks = n // edge
    at_block, pivot_stage, update = elimination(n, table, pivots, factors)
    fetch = pltpu.make_async_copy(effects_hbm, effects_ref, in_sem)
    fetch.start()
    fetch_covar = pltpu.make_async_copy(covar_hbm, covar_ref, covar_sem)
    fetch_covar.start()

    def clear(b, c):
        count_s[b] = 0
        return c

    lax.fori_loop(0, patterns, clear, 0)

    def tally(t, c):
        b = index_ref[t]
        count_s[b] = count_s[b] + 1
        return c

    lax.fori_loop(0, tiles, tally, 0)

    def place(b, state):
        used, offset = state
        many = count_s[b]
        slot_s[used] = b
        start_s[used] = offset
        count_s[b] = offset
        return used + jnp.where(many > 0, 1, 0), offset + many

    used, _ = lax.fori_loop(0, patterns, place, (jnp.int32(0), jnp.int32(0)))
    start_s[used] = tiles

    def sort(t, c):
        b = index_ref[t]
        position = count_s[b]
        order_s[position] = t
        count_s[b] = position + 1
        return c

    lax.fori_loop(0, tiles, sort, 0)
    order_s[tiles] = 0

    weights[...] = jnp.zeros_like(weights)
    stack[...] = jnp.zeros_like(stack)
    chosen = comp_grid_ref[...]
    scale = jnp.zeros(chosen.shape, jnp.float32)
    for g in range(grids):
        scale = jnp.where(chosen == g, grid_ref[g], scale)
    scale = jnp.broadcast_to(scale * scale, (SUB, LANES))
    log_prior = jnp.log(prior_ref[...]) - 0.5 * n * math.log(2.0 * math.pi)

    fetch_covar.wait()

    def columns(t):
        return pl.ds(pl.multiple_of(t * TILE, TILE), TILE)

    def prepare(t, target):
        at = columns(t)
        data = effects_ref[pl.ds(0, even), at]
        x1, x2, x3 = split3(data)
        for piece, part in enumerate((x1, x2, x1, x2, x3)):
            stack[pl.ds(piece * even, even), :] = part.astype(jnp.float32)
        for extra in range(edge_rows):
            line = effects_ref[pl.ds(even + extra, 1), at]
            x1, x2, x3 = split3(line)
            for piece, part in enumerate((x1, x2, x1, x2, x3)):
                stack[pl.ds(PIECES * even + extra * PIECES + piece, 1), :] = part.astype(jnp.float32)
        target[...] = jnp.transpose(stack[...]).astype(jnp.bfloat16)

    def conclude(t, side):
        at = columns(t)
        scores = jnp.transpose(done[...])
        top = jnp.max(scores, axis=0, keepdims=True)
        shifted = jnp.exp(scores - top)
        out_buf[side] = shifted
        peak_ref[0:1, at] = top
        peak_ref[1:2, at] = jnp.sum(shifted, axis=0, keepdims=True)

    def store(t, side):
        return pltpu.make_async_copy(out_buf.at[side], out_hbm.at[:, columns(t)], out_sem.at[side])

    def fill(batch):
        base = batch * SUB
        q = lax.rem(batch, 2)
        for s in range(SUB):
            b = slot_s[jnp.minimum(base + s, used - 1)]
            se_rows[pl.ds(s, 1), :] = se_ref[pl.ds(b, 1), :]
        ses = se_rows[...]
        squares = ses * ses
        for i in range(n):
            noise[pl.ds(i * SUB, SUB), :] = jnp.broadcast_to(squares[:, i : i + 1], (SUB, LANES))

        for rb in range(blocks):
            def fill_row(i, c):
                for j in range(rb * edge, n):
                    table[at_block(q, i, j), :] = covar_ref[pl.ds(i * n + j, SUB, stride=0), :] * scale
                d = at_block(q, i, i)
                table[d, :] = table[d, :] + noise[element(i), :]
                return c

            lax.fori_loop(rb * edge, (rb + 1) * edge, fill_row, 0)

    def advance(q):
        kb = state_s[0]

        @pl.when(state_s[1] >= plan_start[kb + 1])
        def _():
            state_s[0] = kb + 1

            @pl.when(kb + 1 < blocks)
            def _():
                pivot_stage(q, kb + 1)

    def begin(q):
        state_s[0] = 0
        state_s[1] = 0
        pivot_stage(q, 0)

    def drain(q):
        def one_block(kb, c):
            position = state_s[1]

            def one(p, cc):
                update(q, kb, plan_row[p], plan_col[p])
                return cc

            lax.fori_loop(position, plan_end[kb], one, 0)
            state_s[1] = plan_start[kb + 1]

            @pl.when(kb + 1 < blocks)
            def _():
                pivot_stage(q, kb + 1)

            return c

        lax.fori_loop(state_s[0], blocks, one_block, 0)

    def one_batch(batch, carry):
        base = batch * SUB
        q = lax.rem(batch, 2)
        more = base + SUB < used

        @pl.when(batch == 0)
        def _():
            fill(batch)
            begin(q)

        drain(q)
        state_s[0] = blocks
        logs = jnp.zeros((SUB, LANES), jnp.float32)
        for i in range(n):
            d = pivots[pl.ds(i * SUB, SUB), :]
            roots[pl.ds(i * SUB, SUB), :] = lax.rsqrt(d)
            logs = logs + jnp.log(d)
        halfdet[...] = log_prior - 0.5 * logs

        @pl.when(batch == 0)
        def _():
            fetch.wait()
            prepare(order_s[0], following)

        @pl.when(more)
        def _():
            fill(batch + 1)
            begin(1 - q)

        def one_slot(slot, c):
            s = slot - base
            for i in range(n):
                groups = min(i // 16 + 1, even // 16)
                rows = groups * 16
                root = roots[pl.ds(i * SUB + s, SUB, stride=0), :][0:1, :]
                row = table[pl.ds(q * (n + edge) * n * SUB + i * n * SUB + s, rows, stride=SUB), :]
                if i < even:
                    j = lax.broadcasted_iota(jnp.int32, (rows, LANES), 0)
                    row = jnp.where(j < i, row, jnp.where(j == i, 1.0, 0.0))
                row = row * root
                one = row.astype(jnp.bfloat16)
                two = (row - one.astype(jnp.float32)).astype(jnp.bfloat16)
                for piece, part in enumerate((one, one, two, two, one)):
                    weights[i, pl.ds(piece * even, rows), :] = part
                if i >= even:
                    first = root.astype(jnp.bfloat16)
                    second = (root - first.astype(jnp.float32)).astype(jnp.bfloat16)
                    j = lax.broadcasted_iota(jnp.int32, (16, LANES), 0)
                    tail = jnp.zeros((16, LANES), jnp.float32)
                    for piece, part in enumerate((first, first, second, second, first)):
                        tail = jnp.where(j == piece, part.astype(jnp.float32), tail)
                    weights[i, pl.ds(PIECES * even, 16), :] = tail.astype(jnp.bfloat16)
            row_const = halfdet[pl.ds(s, 1), :]

            def one_tile(place_at, cc):
                before = order_s[jnp.maximum(place_at - 1, 0)]
                side = lax.rem(place_at, 2)

                @pl.when(place_at >= 3)
                def _():
                    store(0, 1 - side).wait()

                def body(beside):
                    flipped[...] = following[...]
                    prepare(order_s[place_at + 1], following)
                    conclude(before, 1 - side)
                    for i in range(0, n, 2):
                        if i + 1 < n:
                            right = jnp.concatenate([weights[i], weights[i + 1]], axis=1)
                        else:
                            right = weights[i]
                        white = jnp.dot(flipped[...], right, preferred_element_type=jnp.float32)
                        square = white[:, :LANES] * white[:, :LANES]
                        if i + 1 < n:
                            square = square + white[:, LANES:] * white[:, LANES:]
                        if i:
                            acc[...] += square
                        else:
                            acc[...] = square
                        if beside is not None and i % 10 == 2 and i // 10 < GROUP:
                            beside(i // 10)
                    done[...] = row_const - 0.5 * acc[...]

                kb = state_s[0]
                position = state_s[1]
                working = kb < blocks

                @pl.when(working)
                def _():
                    body(lambda g: update(1 - q, kb, plan_row[position + g], plan_col[position + g]))
                    state_s[1] = position + GROUP
                    advance(1 - q)

                @pl.when(jnp.logical_not(working))
                def _():
                    body(None)

                @pl.when(place_at >= 1)
                def _():
                    store(before, 1 - side).start()

                return cc

            lax.fori_loop(start_s[slot], start_s[slot + 1], one_tile, 0)
            return c

        lax.fori_loop(base, jnp.minimum(used, base + SUB), one_slot, 0)
        return carry

    lax.fori_loop(0, (used + SUB - 1) // SUB, one_batch, 0)
    last = order_s[tiles - 1]
    side = (tiles - 1) % 2
    if tiles >= 3:
        store(0, side).wait()
    conclude(last, side)
    store(last, side).start()
    if tiles >= 2:
        store(0, 1 - side).wait()
    store(last, side).wait()


def shifted_scores(effects, se_table, se_index, covar, grid_scale, comp_grid, weights):
    n, pairs = effects.shape
    patterns = se_table.shape[0]
    tiles = pairs // TILE
    even = n // 16 * 16
    assert covar.shape == (n * n, LANES) and (n - even) * PIECES <= 16
    depth = PIECES * even + 16
    edge = block_edge(n)
    plan = update_plan(n // edge, GROUP)
    vmem = pl.BlockSpec(memory_space=pltpu.VMEM)
    smem = pl.BlockSpec(memory_space=pltpu.SMEM)
    hbm = pl.BlockSpec(memory_space=pl.ANY)
    f32 = jnp.float32
    return pl.pallas_call(
        functools.partial(main_kernel, n, tiles, patterns, grid_scale.shape[0]),
        name="shifted_scores",
        out_shape=(
            jax.ShapeDtypeStruct((LANES, pairs), f32),
            jax.ShapeDtypeStruct((2, pairs), f32),
        ),
        in_specs=[smem] * 6 + [hbm, vmem, hbm, vmem, vmem],
        out_specs=(hbm, vmem),
        scratch_shapes=[
            pltpu.VMEM((2 * (n + edge) * n * SUB, LANES), f32),
            pltpu.VMEM((n * SUB, LANES), f32),
            pltpu.VMEM(((edge * n + edge) * SUB, LANES), f32),
            pltpu.VMEM((n * SUB, LANES), f32),
            pltpu.VMEM((SUB, LANES), f32),
            pltpu.VMEM((n * SUB, LANES), f32),
            pltpu.VMEM((n, depth, LANES), jnp.bfloat16),
            pltpu.VMEM((n, pairs), f32),
            pltpu.VMEM((n * n, LANES), f32),
            pltpu.VMEM((TILE, depth), jnp.bfloat16),
            pltpu.VMEM((TILE, depth), jnp.bfloat16),
            pltpu.VMEM((depth, TILE), f32),
            pltpu.VMEM((TILE, LANES), f32),
            pltpu.VMEM((TILE, LANES), f32),
            pltpu.VMEM((2, LANES, TILE), f32),
            pltpu.VMEM((SUB, n), f32),
            pltpu.SemaphoreType.DMA,
            pltpu.SemaphoreType.DMA,
            pltpu.SemaphoreType.DMA((2,)),
            pltpu.SMEM((patterns + 1,), jnp.int32),
            pltpu.SMEM((patterns + 1,), jnp.int32),
            pltpu.SMEM((patterns + 1,), jnp.int32),
            pltpu.SMEM((tiles + 1,), jnp.int32),
            pltpu.SMEM((2,), jnp.int32),
        ],
        compiler_params=pltpu.CompilerParams(vmem_limit_bytes=40 * 1024 * 1024),
    )(se_index, grid_scale, *plan, effects, se_table, covar, comp_grid[None], weights[None])


def exact_dot(left, right, dims):
    return lax.dot_general(left, right, (dims, ((), ())), precision=lax.Precision.HIGHEST, preferred_element_type=jnp.float32)


def finish_kernel(width, shifted_ref, own_ref, peaks_ref, out_hbm, loglik_ref, mass_ref, buffer, sems):
    pairs = shifted_ref.shape[1]
    steps = pairs // width
    copies = []
    partial = None
    for step in range(steps):
        at = pl.ds(step * width, width)
        tops = [peaks_ref[c, 0:1, at] for c in range(peaks_ref.shape[0])]
        sums = [peaks_ref[c, 1:2, at] for c in range(peaks_ref.shape[0])]
        top = functools.reduce(jnp.maximum, tops)
        total = sum(s * jnp.exp(t - top) for s, t in zip(sums, tops))
        loglik = top + jnp.log(total)
        loglik_ref[:, at] = loglik
        factor = jnp.exp(own_ref[0:1, at] - loglik)
        for c in range(width // LANES):
            lanes = pl.ds(step * width + c * LANES, LANES)
            value = shifted_ref[:, lanes] * factor[:, c * LANES : (c + 1) * LANES]
            buffer[:, lanes] = value
            partial = value if partial is None else partial + value
        copy = pltpu.make_async_copy(buffer.at[:, at], out_hbm.at[:, at], sems.at[step])
        copy.start()
        copies.append(copy)
    mass = jnp.sum(jnp.transpose(partial), axis=0, keepdims=True)
    mass_ref[...] = jnp.broadcast_to(mass, mass_ref.shape)
    for copy in copies:
        copy.wait()


def finish(shifted, peak, peaks, receivers):
    comps, pairs = shifted.shape
    width = min(pairs, 1024)
    vmem = pl.BlockSpec(memory_space=pltpu.VMEM)
    return pl.pallas_call(
        functools.partial(finish_kernel, width),
        name="finish",
        in_specs=[vmem, vmem, vmem],
        out_specs=(pl.BlockSpec(memory_space=pl.ANY), vmem, vmem),
        out_shape=(
            jax.ShapeDtypeStruct((comps, pairs), jnp.float32),
            jax.ShapeDtypeStruct((1, pairs), jnp.float32),
            jax.ShapeDtypeStruct((receivers, comps), jnp.float32),
        ),
        scratch_shapes=[pltpu.VMEM((comps, pairs), jnp.float32), pltpu.SemaphoreType.DMA((pairs // width,))],
        compiler_params=pltpu.CompilerParams(vmem_limit_bytes=12 * 1024 * 1024),
    )(shifted, peak, peaks)


def per_device(effects, se_table, se_index, base_root, grid_scale, comp_base, comp_grid, weights):
    n, pairs = effects.shape
    comps = comp_base.shape[0]
    covariances = jnp.einsum("uij,ukj->uik", base_root, base_root, precision=lax.Precision.HIGHEST)
    covariances = covariances.reshape(covariances.shape[0], n * n)
    bases = jnp.arange(covariances.shape[0], dtype=jnp.int32)
    pick = (comp_base[None] == bases[:, None]).astype(jnp.float32)
    covar = exact_dot(covariances, pick, ((0,), (0,)))
    shifted, peak = shifted_scores(effects, se_table, se_index, covar, grid_scale, comp_grid, weights)
    peaks = lax.all_gather(peak, "comp")
    receivers = lax.axis_size("pairs")
    responsibility, loglik, mass = finish(shifted, peak, peaks, receivers)
    masses = jnp.sum(lax.all_to_all(mass, "pairs", 0, 0, tiled=True), axis=0)
    all_pairs = pairs * lax.axis_size("pairs")
    all_comps = comps * lax.axis_size("comp")
    log_weights = jnp.log((masses + 1.0) / (all_pairs + all_comps))
    return (responsibility, log_weights, loglik[0])


def solution(mesh):
    placed = (P(None, "pairs"), P(), P("pairs"), P(), P(), P("comp"), P("comp"), P("comp"))
    return jax.shard_map(
        per_device,
        mesh=mesh,
        in_specs=placed,
        out_specs=(P("comp", "pairs"), P("comp"), P("pairs")),
        check_vma=False,
    )
```

```python
import functools
import math

import jax
import jax.numpy as jnp
import numpy as np
from jax import lax
from jax.experimental import pallas as pl
from jax.experimental.pallas import tpu as pltpu
from jax.sharding import PartitionSpec as P

TILE = 512
SUB = 8
LANES = 128
PIECES = 5
GROUP = 5
ROWS = 3
HEAD = 15
SPAN = 16


def block_edge(count):
    return max(edge for edge in range(1, 9) if count % edge == 0)


def element(index):
    return pl.ds(pl.multiple_of(index * SUB, SUB), SUB)


def update_plan(blocks, group):
    lists = []
    for kb in range(blocks):
        pairs = [(ib, jb) for ib in range(kb + 1, blocks) for jb in list(range(kb)) + list(range(ib + 1, blocks))]
        while len(pairs) % group:
            pairs.append((blocks, 0))
        lists.append(pairs)
    flat = [pair for pairs in lists for pair in pairs]
    starts = np.cumsum([0] + [len(pairs) for pairs in lists])
    return tuple(np.array(a, np.int32) for a in ([p[0] for p in flat], [p[1] for p in flat], starts))


def elimination(n, table, pivots, factors):
    edge = block_edge(n)
    blocks = n // edge

    def at(q, i, j):
        return element(q * (n + edge) * n + i * n + j)

    def pivot_stage(q, kb):
        first = kb * edge
        diag = [[table[at(q, first + m, first + j), :] if j >= m else None for j in range(edge)] for m in range(edge)]
        lower = [[None] * edge for _ in range(edge)]
        inverse = [[None] * edge for _ in range(edge)]
        recips = []
        for m in range(edge):
            d = diag[m][m]
            recip = 1.0 / d
            recips.append(recip)
            pivots[element(first + m), :] = d
            for r in range(m + 1, edge):
                lower[r][m] = diag[m][r] * recip
            for r in range(m + 1, edge):
                for j in range(r, edge):
                    diag[r][j] = diag[r][j] - lower[r][m] * diag[m][j]
                for j in range(m):
                    inverse[r][j] = inverse[r][j] - lower[r][m] * inverse[m][j]
                inverse[r][m] = -lower[r][m]
        for r in range(edge):
            for j in range(r):
                table[at(q, first + r, first + j), :] = inverse[r][j]

        def column_block(jb, with_factor):
            col = jb * edge
            for j in range(edge):
                rows = [table[at(q, first + m, col + j), :] for m in range(edge)]
                for m in range(edge):
                    for r in range(m + 1, edge):
                        rows[r] = rows[r] - lower[r][m] * rows[m]
                for m in range(edge):
                    if m:
                        table[at(q, first + m, col + j), :] = rows[m]
                    if with_factor:
                        factors[element(m * n + col + j), :] = rows[m] * recips[m]

        def left(jb, c):
            column_block(jb, False)
            return c

        def right(jb, c):
            column_block(jb, True)
            return c

        lax.fori_loop(0, kb, left, 0)
        lax.fori_loop(kb + 1, blocks, right, 0)

        def row_block(ib, c):
            row = ib * edge
            for start in range(0, edge, ROWS):
                rows = range(start, min(start + ROWS, edge))
                size = len(rows)
                f = [[factors[element(m * n + row + i), :] for m in range(edge)] for i in rows]
                totals = [list(line) for line in f]
                for m in range(1, edge):
                    for j in range(m):
                        v = table[at(q, first + m, first + j), :]
                        for a in range(size):
                            totals[a][j] = totals[a][j] + f[a][m] * v
                values = {}
                for j in range(rows[0], edge):
                    live = [a for a, i in enumerate(rows) if i <= j]
                    for a in live:
                        values[a, j] = table[at(q, row + rows[a], row + j), :]
                    for m in range(edge):
                        u = table[at(q, first + m, row + j), :]
                        for a in live:
                            values[a, j] = values[a, j] - f[a][m] * u
                for a, i in enumerate(rows):
                    for j in range(edge):
                        table[at(q, row + i, first + j), :] = -totals[a][j]
                for (a, j), v in values.items():
                    table[at(q, row + rows[a], row + j), :] = v

            return c

        lax.fori_loop(kb + 1, blocks, row_block, 0)

    def update(q, kb, ib, jb):
        first, row, col = kb * edge, ib * edge, jb * edge
        start = 0
        for size in (edge - edge // 2, edge // 2):
            rows = range(start, start + size)
            start += size
            held = [[table[at(q, row + i, col + j), :] for j in range(edge)] for i in rows]
            for m in range(edge):
                f = [factors[element(m * n + row + i), :] for i in rows]
                for j in range(edge):
                    u = table[at(q, first + m, col + j), :]
                    for a in range(len(f)):
                        held[a][j] = held[a][j] - f[a] * u
            for a, i in enumerate(rows):
                for j in range(edge):
                    table[at(q, row + i, col + j), :] = held[a][j]

    return at, pivot_stage, update


def split3(value):
    one = value.astype(jnp.bfloat16)
    rest = value - one.astype(jnp.float32)
    two = rest.astype(jnp.bfloat16)
    three = (rest - two.astype(jnp.float32)).astype(jnp.bfloat16)
    return one, two, three


def main_kernel(
    n, tiles, patterns, grids,
    index_ref, grid_ref, plan_row, plan_col, plan_start, effects_hbm, se_ref, covar_hbm, comp_grid_ref, prior_ref,
    out_hbm, peak_ref,
    table, pivots, factors, roots, halfdet, noise, weights, effects_ref, covar_ref, flipped, following, stack, acc, done, out_buf, se_rows,
    scaled, forms, form_weights, doubled, products, features,
    in_sem, covar_sem, out_sem,
    count_s, start_s, slot_s, order_s, state_s,
):
    even = n // 16 * 16
    edge_rows = n - even
    edge = block_edge(n)
    blocks = n // edge
    at_block, pivot_stage, update = elimination(n, table, pivots, factors)
    fetch = pltpu.make_async_copy(effects_hbm, effects_ref, in_sem)
    fetch.start()
    fetch_covar = pltpu.make_async_copy(covar_hbm, covar_ref, covar_sem)
    fetch_covar.start()

    def clear(b, c):
        count_s[b] = 0
        return c

    lax.fori_loop(0, patterns, clear, 0)

    def tally(t, c):
        b = index_ref[t]
        count_s[b] = count_s[b] + 1
        return c

    lax.fori_loop(0, tiles, tally, 0)

    def place(b, state):
        used, offset = state
        many = count_s[b]
        slot_s[used] = b
        start_s[used] = offset
        count_s[b] = offset
        return used + jnp.where(many > 0, 1, 0), offset + many

    used, _ = lax.fori_loop(0, patterns, place, (jnp.int32(0), jnp.int32(0)))
    start_s[used] = tiles

    def sort(t, c):
        b = index_ref[t]
        position = count_s[b]
        order_s[position] = t
        count_s[b] = position + 1
        return c

    lax.fori_loop(0, tiles, sort, 0)
    order_s[tiles] = 0

    weights[...] = jnp.zeros_like(weights)
    stack[...] = jnp.zeros_like(stack)
    forms[...] = jnp.zeros_like(forms)
    doubled[...] = jnp.zeros_like(doubled)
    chosen = comp_grid_ref[...]
    scale = jnp.zeros(chosen.shape, jnp.float32)
    for g in range(grids):
        scale = jnp.where(chosen == g, grid_ref[g], scale)
    scale = jnp.broadcast_to(scale * scale, (SUB, LANES))
    log_prior = jnp.log(prior_ref[...]) - 0.5 * n * math.log(2.0 * math.pi)

    fetch_covar.wait()

    def columns(t):
        return pl.ds(pl.multiple_of(t * TILE, TILE), TILE)

    def head_forms(q):
        def line(i, a):
            return pl.ds((i * HEAD + a) * SUB, SUB)

        for i in range(HEAD):
            root = roots[pl.ds(i * SUB, SUB), :]
            for a in range(i):
                scaled[line(i, a), :] = table[at_block(q, i, a), :] * root
            scaled[line(i, i), :] = root
        for a in range(HEAD):
            own = {i: scaled[line(i, a), :] for i in range(a, HEAD)}
            for b in range(a + 1):
                total = None
                for i in range(a, HEAD):
                    term = own[i] * scaled[line(i, b), :]
                    total = term if total is None else total + term
                gap = a - b
                d, j = (gap, b) if gap <= HEAD // 2 else (HEAD - gap, a)
                forms[pl.ds((d * SPAN + j) * SUB, SUB), :] = total if gap == 0 else 2.0 * total

    def head_features(t):
        at = columns(t)
        x = effects_ref[pl.ds(0, SPAN), at]
        doubled[pl.ds(0, SPAN), :] = x
        doubled[pl.ds(HEAD, SPAN), :] = x
        j = lax.broadcasted_iota(jnp.int32, x.shape, 0)
        x = jnp.where(j < HEAD, x, 0.0)
        for d in range(LANES // SPAN):
            products[pl.ds(d * SPAN, SPAN), :] = x * doubled[pl.ds(d, SPAN), :]
        for piece, part in enumerate(split3(jnp.transpose(products[...]))):
            features[:, piece * LANES : (piece + 1) * LANES] = part

    def head_norm():
        f = [features[:, p * LANES : (p + 1) * LANES] for p in range(3)]
        w = [form_weights[pl.ds(p * LANES, LANES), :] for p in range(3)]
        left = jnp.concatenate([f[0], f[0], f[1], f[1], f[0], f[2]], axis=1)
        right = jnp.concatenate([w[0], w[1], w[0], w[1], w[2], w[0]], axis=0)
        return jnp.dot(left, right, preferred_element_type=jnp.float32)

    def prepare(t, target):
        at = columns(t)
        data = effects_ref[pl.ds(0, even), at]
        x1, x2, x3 = split3(data)
        for piece, part in enumerate((x1, x2, x1, x2, x3)):
            stack[pl.ds(piece * even, even), :] = part.astype(jnp.float32)
        for extra in range(edge_rows):
            line = effects_ref[pl.ds(even + extra, 1), at]
            x1, x2, x3 = split3(line)
            for piece, part in enumerate((x1, x2, x1, x2, x3)):
                stack[pl.ds(PIECES * even + extra * PIECES + piece, 1), :] = part.astype(jnp.float32)
        target[...] = jnp.transpose(stack[...]).astype(jnp.bfloat16)

    def conclude(t, side):
        at = columns(t)
        scores = jnp.transpose(done[...])
        top = jnp.max(scores, axis=0, keepdims=True)
        shifted = jnp.exp(scores - top)
        out_buf[side] = shifted
        peak_ref[0:1, at] = top
        peak_ref[1:2, at] = jnp.sum(shifted, axis=0, keepdims=True)

    def store(t, side):
        return pltpu.make_async_copy(out_buf.at[side], out_hbm.at[:, columns(t)], out_sem.at[side])

    def fill(batch):
        base = batch * SUB
        q = lax.rem(batch, 2)
        for s in range(SUB):
            b = slot_s[jnp.minimum(base + s, used - 1)]
            se_rows[pl.ds(s, 1), :] = se_ref[pl.ds(b, 1), :]
        ses = se_rows[...]
        squares = ses * ses
        for i in range(n):
            noise[pl.ds(i * SUB, SUB), :] = jnp.broadcast_to(squares[:, i : i + 1], (SUB, LANES))

        for rb in range(blocks):
            def fill_row(i, c):
                for j in range(rb * edge, n):
                    table[at_block(q, i, j), :] = covar_ref[pl.ds(i * n + j, SUB, stride=0), :] * scale
                d = at_block(q, i, i)
                table[d, :] = table[d, :] + noise[element(i), :]
                return c

            lax.fori_loop(rb * edge, (rb + 1) * edge, fill_row, 0)

    def advance(q):
        kb = state_s[0]

        @pl.when(state_s[1] >= plan_start[kb + 1])
        def _():
            state_s[0] = kb + 1

            @pl.when(kb + 1 < blocks)
            def _():
                pivot_stage(q, kb + 1)

    def begin(q):
        state_s[0] = 0
        state_s[1] = 0
        pivot_stage(q, 0)

    def drain(q):
        def one_block(kb, c):
            position = state_s[1]

            def some(p, cc):
                for g in range(GROUP):
                    update(q, kb, plan_row[position + p * GROUP + g], plan_col[position + p * GROUP + g])
                return cc

            lax.fori_loop(0, (plan_start[kb + 1] - position) // GROUP, some, 0)
            state_s[1] = plan_start[kb + 1]

            @pl.when(kb + 1 < blocks)
            def _():
                pivot_stage(q, kb + 1)

            return c

        lax.fori_loop(state_s[0], blocks, one_block, 0)

    def one_batch(batch, carry):
        base = batch * SUB
        q = lax.rem(batch, 2)
        more = base + SUB < used

        @pl.when(batch == 0)
        def _():
            fill(batch)
            begin(q)

        drain(q)
        state_s[0] = blocks
        logs = jnp.zeros((SUB, LANES), jnp.float32)
        for i in range(n):
            d = pivots[pl.ds(i * SUB, SUB), :]
            roots[pl.ds(i * SUB, SUB), :] = lax.rsqrt(d)
            logs = logs + jnp.log(d)
        halfdet[...] = log_prior - 0.5 * logs
        head_forms(q)

        @pl.when(batch == 0)
        def _():
            fetch.wait()
            prepare(order_s[0], following)

        @pl.when(more)
        def _():
            fill(batch + 1)
            begin(1 - q)

        def one_slot(slot, c):
            s = slot - base
            for piece, part in enumerate(split3(forms[pl.ds(s, LANES, stride=SUB), :])):
                form_weights[pl.ds(piece * LANES, LANES), :] = part
            for i in range(HEAD, n):
                groups = min(i // 16 + 1, even // 16)
                rows = groups * 16
                root = roots[pl.ds(i * SUB + s, SUB, stride=0), :][0:1, :]
                row = table[pl.ds(q * (n + edge) * n * SUB + i * n * SUB + s, rows, stride=SUB), :]
                if i < even:
                    j = lax.broadcasted_iota(jnp.int32, (rows, LANES), 0)
                    row = jnp.where(j < i, row, jnp.where(j == i, 1.0, 0.0))
                row = row * root
                one = row.astype(jnp.bfloat16)
                two = (row - one.astype(jnp.float32)).astype(jnp.bfloat16)
                weights[i, pl.ds(0, rows), :] = one
                weights[i, pl.ds(even, rows), :] = two
                if i >= even:
                    first = root.astype(jnp.bfloat16)
                    second = (root - first.astype(jnp.float32)).astype(jnp.bfloat16)
                    j = lax.broadcasted_iota(jnp.int32, (16, LANES), 0)
                    tail = jnp.zeros((16, LANES), jnp.float32)
                    for piece, part in enumerate((first, first, second, second, first)):
                        tail = jnp.where(j == piece, part.astype(jnp.float32), tail)
                    weights[i, pl.ds(2 * even, 16), :] = tail.astype(jnp.bfloat16)
            row_const = halfdet[pl.ds(s, 1), :]

            def operand(i):
                one = weights[i, pl.ds(0, even), :]
                two = weights[i, pl.ds(even, even), :]
                return jnp.concatenate([one, one, two, two, one, weights[i, pl.ds(2 * even, 16), :]], axis=0)

            def one_tile(place_at, cc):
                before = order_s[jnp.maximum(place_at - 1, 0)]
                side = lax.rem(place_at, 2)

                @pl.when(place_at >= 3)
                def _():
                    store(0, 1 - side).wait()

                def body(beside):
                    flipped[...] = following[...]
                    prepare(order_s[place_at + 1], following)
                    conclude(before, 1 - side)
                    head_features(order_s[place_at])
                    for i in range(HEAD, n, 2):
                        right = jnp.concatenate([operand(r) for r in range(i, min(i + 2, n))], axis=1)
                        white = jnp.dot(flipped[...], right, preferred_element_type=jnp.float32)
                        square = white[:, :LANES] * white[:, :LANES]
                        if i + 1 < n:
                            square = square + white[:, LANES:] * white[:, LANES:]
                        if i > HEAD:
                            acc[...] += square
                        else:
                            acc[...] = square
                        if beside is not None:
                            for g in range(GROUP):
                                if (2 * g + 1) * (n - HEAD) // (2 * GROUP) // 2 == (i - HEAD) // 2:
                                    beside(g)
                    done[...] = row_const - 0.5 * (acc[...] + head_norm())

                kb = state_s[0]
                position = state_s[1]
                working = kb < blocks

                @pl.when(working)
                def _():
                    body(lambda g: update(1 - q, kb, plan_row[position + g], plan_col[position + g]))
                    state_s[1] = position + GROUP
                    advance(1 - q)

                @pl.when(jnp.logical_not(working))
                def _():
                    body(None)

                @pl.when(place_at >= 1)
                def _():
                    store(before, 1 - side).start()

                return cc

            lax.fori_loop(start_s[slot], start_s[slot + 1], one_tile, 0)
            return c

        lax.fori_loop(base, jnp.minimum(used, base + SUB), one_slot, 0)
        return carry

    lax.fori_loop(0, (used + SUB - 1) // SUB, one_batch, 0)
    last = order_s[tiles - 1]
    side = (tiles - 1) % 2
    if tiles >= 3:
        store(0, side).wait()
    conclude(last, side)
    store(last, side).start()
    if tiles >= 2:
        store(0, 1 - side).wait()
    store(last, side).wait()


def shifted_scores(effects, se_table, se_index, covar, grid_scale, comp_grid, weights):
    n, pairs = effects.shape
    patterns = se_table.shape[0]
    tiles = pairs // TILE
    even = n // 16 * 16
    assert covar.shape == (n * n, LANES) and (n - even) * PIECES <= 16
    depth = PIECES * even + 16
    edge = block_edge(n)
    plan = update_plan(n // edge, GROUP)
    vmem = pl.BlockSpec(memory_space=pltpu.VMEM)
    smem = pl.BlockSpec(memory_space=pltpu.SMEM)
    hbm = pl.BlockSpec(memory_space=pl.ANY)
    f32 = jnp.float32
    return pl.pallas_call(
        functools.partial(main_kernel, n, tiles, patterns, grid_scale.shape[0]),
        name="shifted_scores",
        out_shape=(
            jax.ShapeDtypeStruct((LANES, pairs), f32),
            jax.ShapeDtypeStruct((2, pairs), f32),
        ),
        in_specs=[smem] * 5 + [hbm, vmem, hbm, vmem, vmem],
        out_specs=(hbm, vmem),
        scratch_shapes=[
            pltpu.VMEM((2 * (n + edge) * n * SUB, LANES), f32),
            pltpu.VMEM((n * SUB, LANES), f32),
            pltpu.VMEM(((edge * n + edge) * SUB, LANES), f32),
            pltpu.VMEM((n * SUB, LANES), f32),
            pltpu.VMEM((SUB, LANES), f32),
            pltpu.VMEM((n * SUB, LANES), f32),
            pltpu.VMEM((n, 2 * even + 16, LANES), jnp.bfloat16),
            pltpu.VMEM((n, pairs), f32),
            pltpu.VMEM((n * n, LANES), f32),
            pltpu.VMEM((TILE, depth), jnp.bfloat16),
            pltpu.VMEM((TILE, depth), jnp.bfloat16),
            pltpu.VMEM((depth, TILE), f32),
            pltpu.VMEM((TILE, LANES), f32),
            pltpu.VMEM((TILE, LANES), f32),
            pltpu.VMEM((2, LANES, TILE), f32),
            pltpu.VMEM((SUB, n), f32),
            pltpu.VMEM((HEAD * HEAD * SUB, LANES), f32),
            pltpu.VMEM((LANES * SUB, LANES), f32),
            pltpu.VMEM((3 * LANES, LANES), jnp.bfloat16),
            pltpu.VMEM((2 * SPAN, TILE), f32),
            pltpu.VMEM((LANES, TILE), f32),
            pltpu.VMEM((TILE, 3 * LANES), jnp.bfloat16),
            pltpu.SemaphoreType.DMA,
            pltpu.SemaphoreType.DMA,
            pltpu.SemaphoreType.DMA((2,)),
            pltpu.SMEM((patterns + 1,), jnp.int32),
            pltpu.SMEM((patterns + 1,), jnp.int32),
            pltpu.SMEM((patterns + 1,), jnp.int32),
            pltpu.SMEM((tiles + 1,), jnp.int32),
            pltpu.SMEM((2,), jnp.int32),
        ],
        compiler_params=pltpu.CompilerParams(vmem_limit_bytes=40 * 1024 * 1024),
    )(se_index, grid_scale, *plan, effects, se_table, covar, comp_grid[None], weights[None])


def exact_dot(left, right, dims):
    return lax.dot_general(left, right, (dims, ((), ())), precision=lax.Precision.HIGHEST, preferred_element_type=jnp.float32)


def finish_kernel(width, shifted_ref, own_ref, peaks_ref, out_hbm, loglik_ref, mass_ref, buffer, sems):
    pairs = shifted_ref.shape[1]
    steps = pairs // width
    copies = []
    partial = None
    for step in range(steps):
        at = pl.ds(step * width, width)
        tops = [peaks_ref[c, 0:1, at] for c in range(peaks_ref.shape[0])]
        sums = [peaks_ref[c, 1:2, at] for c in range(peaks_ref.shape[0])]
        top = functools.reduce(jnp.maximum, tops)
        total = sum(s * jnp.exp(t - top) for s, t in zip(sums, tops))
        loglik = top + jnp.log(total)
        loglik_ref[:, at] = loglik
        factor = jnp.exp(own_ref[0:1, at] - loglik)
        for c in range(width // LANES):
            lanes = pl.ds(step * width + c * LANES, LANES)
            value = shifted_ref[:, lanes] * factor[:, c * LANES : (c + 1) * LANES]
            buffer[:, lanes] = value
            partial = value if partial is None else partial + value
        copy = pltpu.make_async_copy(buffer.at[:, at], out_hbm.at[:, at], sems.at[step])
        copy.start()
        copies.append(copy)
    mass = jnp.sum(jnp.transpose(partial), axis=0, keepdims=True)
    mass_ref[...] = jnp.broadcast_to(mass, mass_ref.shape)
    for copy in copies:
        copy.wait()


def finish(shifted, peak, peaks, receivers):
    comps, pairs = shifted.shape
    width = min(pairs, 1024)
    vmem = pl.BlockSpec(memory_space=pltpu.VMEM)
    return pl.pallas_call(
        functools.partial(finish_kernel, width),
        name="finish",
        in_specs=[vmem, vmem, vmem],
        out_specs=(pl.BlockSpec(memory_space=pl.ANY), vmem, vmem),
        out_shape=(
            jax.ShapeDtypeStruct((comps, pairs), jnp.float32),
            jax.ShapeDtypeStruct((1, pairs), jnp.float32),
            jax.ShapeDtypeStruct((receivers, comps), jnp.float32),
        ),
        scratch_shapes=[pltpu.VMEM((comps, pairs), jnp.float32), pltpu.SemaphoreType.DMA((pairs // width,))],
        compiler_params=pltpu.CompilerParams(vmem_limit_bytes=12 * 1024 * 1024),
    )(shifted, peak, peaks)


def per_device(effects, se_table, se_index, base_root, grid_scale, comp_base, comp_grid, weights):
    n, pairs = effects.shape
    comps = comp_base.shape[0]
    covariances = jnp.einsum("uij,ukj->uik", base_root, base_root, precision=lax.Precision.HIGHEST)
    covariances = covariances.reshape(covariances.shape[0], n * n)
    bases = jnp.arange(covariances.shape[0], dtype=jnp.int32)
    pick = (comp_base[None] == bases[:, None]).astype(jnp.float32)
    covar = exact_dot(covariances, pick, ((0,), (0,)))
    shifted, peak = shifted_scores(effects, se_table, se_index, covar, grid_scale, comp_grid, weights)
    peaks = lax.all_gather(peak, "comp")
    receivers = lax.axis_size("pairs")
    responsibility, loglik, mass = finish(shifted, peak, peaks, receivers)
    masses = jnp.sum(lax.all_to_all(mass, "pairs", 0, 0, tiled=True), axis=0)
    all_pairs = pairs * lax.axis_size("pairs")
    all_comps = comps * lax.axis_size("comp")
    log_weights = jnp.log((masses + 1.0) / (all_pairs + all_comps))
    return (responsibility, log_weights, loglik[0])


def solution(mesh):
    placed = (P(None, "pairs"), P(), P("pairs"), P(), P(), P("comp"), P("comp"), P("comp"))
    return jax.shard_map(
        per_device,
        mesh=mesh,
        in_specs=placed,
        out_specs=(P("comp", "pairs"), P("comp"), P("pairs")),
        check_vma=False,
    )
```

```python
import functools
import math

import jax
import jax.numpy as jnp
import numpy as np
from jax import lax
from jax.experimental import pallas as pl
from jax.experimental.pallas import tpu as pltpu
from jax.sharding import PartitionSpec as P

TILE = 512
SUB = 8
LANES = 128
PIECES = 5
GROUP = 5
ROWS = 3
HEAD = 15
SPAN = 16


def block_edge(count):
    return max(edge for edge in range(1, 9) if count % edge == 0)


def element(index):
    return pl.ds(pl.multiple_of(index * SUB, SUB), SUB)


def update_plan(blocks, group):
    lists = []
    for kb in range(blocks):
        pairs = [(ib, jb) for ib in range(kb + 1, blocks) for jb in list(range(kb)) + list(range(ib + 1, blocks))]
        while len(pairs) % group:
            pairs.append((blocks, 0))
        lists.append(pairs)
    flat = [pair for pairs in lists for pair in pairs]
    starts = np.cumsum([0] + [len(pairs) for pairs in lists])
    return tuple(np.array(a, np.int32) for a in ([p[0] for p in flat], [p[1] for p in flat], starts))


def elimination(n, table, pivots, factors):
    edge = block_edge(n)
    blocks = n // edge

    def at(q, i, j):
        return element(q * (n + edge) * n + i * n + j)

    def pivot_stage(q, kb):
        first = kb * edge
        diag = [[table[at(q, first + m, first + j), :] if j >= m else None for j in range(edge)] for m in range(edge)]
        lower = [[None] * edge for _ in range(edge)]
        inverse = [[None] * edge for _ in range(edge)]
        recips = []
        for m in range(edge):
            d = diag[m][m]
            recip = 1.0 / d
            recips.append(recip)
            pivots[element(first + m), :] = d
            for r in range(m + 1, edge):
                lower[r][m] = diag[m][r] * recip
            for r in range(m + 1, edge):
                for j in range(r, edge):
                    diag[r][j] = diag[r][j] - lower[r][m] * diag[m][j]
                for j in range(m):
                    inverse[r][j] = inverse[r][j] - lower[r][m] * inverse[m][j]
                inverse[r][m] = -lower[r][m]
        for r in range(edge):
            for j in range(r):
                table[at(q, first + r, first + j), :] = inverse[r][j]

        def column_block(jb, with_factor):
            col = jb * edge
            for j in range(edge):
                rows = [table[at(q, first + m, col + j), :] for m in range(edge)]
                for m in range(edge):
                    for r in range(m + 1, edge):
                        rows[r] = rows[r] - lower[r][m] * rows[m]
                for m in range(edge):
                    if m:
                        table[at(q, first + m, col + j), :] = rows[m]
                    if with_factor:
                        factors[element(m * n + col + j), :] = rows[m] * recips[m]

        def left(jb, c):
            column_block(jb, False)
            return c

        def right(jb, c):
            column_block(jb, True)
            return c

        lax.fori_loop(0, kb, left, 0)
        lax.fori_loop(kb + 1, blocks, right, 0)

        def row_block(ib, c):
            row = ib * edge
            for start in range(0, edge, ROWS):
                rows = range(start, min(start + ROWS, edge))
                size = len(rows)
                f = [[factors[element(m * n + row + i), :] for m in range(edge)] for i in rows]
                totals = [list(line) for line in f]
                for m in range(1, edge):
                    for j in range(m):
                        v = table[at(q, first + m, first + j), :]
                        for a in range(size):
                            totals[a][j] = totals[a][j] + f[a][m] * v
                values = {}
                for j in range(rows[0], edge):
                    live = [a for a, i in enumerate(rows) if i <= j]
                    for a in live:
                        values[a, j] = table[at(q, row + rows[a], row + j), :]
                    for m in range(edge):
                        u = table[at(q, first + m, row + j), :]
                        for a in live:
                            values[a, j] = values[a, j] - f[a][m] * u
                for a, i in enumerate(rows):
                    for j in range(edge):
                        table[at(q, row + i, first + j), :] = -totals[a][j]
                for (a, j), v in values.items():
                    table[at(q, row + rows[a], row + j), :] = v

            return c

        lax.fori_loop(kb + 1, blocks, row_block, 0)

    def update(q, kb, ib, jb):
        first, row, col = kb * edge, ib * edge, jb * edge
        start = 0
        for size in (edge - edge // 2, edge // 2):
            rows = range(start, start + size)
            start += size
            held = [[table[at(q, row + i, col + j), :] for j in range(edge)] for i in rows]
            for m in range(edge):
                f = [factors[element(m * n + row + i), :] for i in rows]
                for j in range(edge):
                    u = table[at(q, first + m, col + j), :]
                    for a in range(len(f)):
                        held[a][j] = held[a][j] - f[a] * u
            for a, i in enumerate(rows):
                for j in range(edge):
                    table[at(q, row + i, col + j), :] = held[a][j]

    return at, pivot_stage, update


def split3(value):
    one = value.astype(jnp.bfloat16)
    rest = value - one.astype(jnp.float32)
    two = rest.astype(jnp.bfloat16)
    three = (rest - two.astype(jnp.float32)).astype(jnp.bfloat16)
    return one, two, three


def main_kernel(
    n, tiles, patterns, grids,
    index_ref, grid_ref, plan_row, plan_col, plan_start, effects_hbm, se_ref, root_ref, comp_base_ref, comp_grid_ref, prior_ref,
    out_hbm, peak_ref,
    table, pivots, factors, roots, halfdet, noise, weights, effects_ref, base_covar, covar_ref, flipped, following, stack, acc, done, out_buf, se_rows,
    scaled, forms, form_weights, doubled, products, features,
    in_sem, out_sem,
    count_s, start_s, slot_s, order_s, state_s,
):
    even = n // 16 * 16
    edge_rows = n - even
    edge = block_edge(n)
    blocks = n // edge
    at_block, pivot_stage, update = elimination(n, table, pivots, factors)
    fetch = pltpu.make_async_copy(effects_hbm, effects_ref, in_sem)
    fetch.start()

    def clear(b, c):
        count_s[b] = 0
        return c

    lax.fori_loop(0, patterns, clear, 0)

    def tally(t, c):
        b = index_ref[t]
        count_s[b] = count_s[b] + 1
        return c

    lax.fori_loop(0, tiles, tally, 0)

    def place(b, state):
        used, offset = state
        many = count_s[b]
        slot_s[used] = b
        start_s[used] = offset
        count_s[b] = offset
        return used + jnp.where(many > 0, 1, 0), offset + many

    used, _ = lax.fori_loop(0, patterns, place, (jnp.int32(0), jnp.int32(0)))
    start_s[used] = tiles

    def sort(t, c):
        b = index_ref[t]
        position = count_s[b]
        order_s[position] = t
        count_s[b] = position + 1
        return c

    lax.fori_loop(0, tiles, sort, 0)
    order_s[tiles] = 0

    weights[...] = jnp.zeros_like(weights)
    stack[...] = jnp.zeros_like(stack)
    forms[...] = jnp.zeros_like(forms)
    doubled[...] = jnp.zeros_like(doubled)
    chosen = comp_grid_ref[...]
    scale = jnp.zeros(chosen.shape, jnp.float32)
    for g in range(grids):
        scale = jnp.where(chosen == g, grid_ref[g], scale)
    scale = jnp.broadcast_to(scale * scale, (SUB, LANES))
    log_prior = jnp.log(prior_ref[...]) - 0.5 * n * math.log(2.0 * math.pi)

    bases = root_ref.shape[0]
    rows_up = (n + SUB - 1) // SUB * SUB
    for u in range(bases):
        root = root_ref[u]
        base_covar[pl.ds(u * rows_up, n), 0:n] = lax.dot_general(
            root, root, (((1,), (1,)), ((), ())), precision=lax.Precision.HIGHEST, preferred_element_type=jnp.float32
        )
    pick = lax.broadcasted_iota(jnp.int32, (bases, LANES), 0) == comp_base_ref[...]
    pick = jnp.where(pick, 1.0, 0.0).astype(jnp.bfloat16)
    pick = jnp.concatenate([pick, pick, pick], axis=0)
    for i in range(n):
        lines = jnp.concatenate(split3(base_covar[pl.ds(i, bases, stride=rows_up), :]), axis=0)
        picked = lax.dot_general(lines, pick, (((0,), (0,)), ((), ())), preferred_element_type=jnp.float32)
        covar_ref[pl.ds(i * rows_up, rows_up), :] = picked[:rows_up]

    def columns(t):
        return pl.ds(pl.multiple_of(t * TILE, TILE), TILE)

    def head_forms(q):
        def line(i, a):
            return pl.ds((i * HEAD + a) * SUB, SUB)

        for i in range(HEAD):
            root = roots[pl.ds(i * SUB, SUB), :]
            for a in range(i):
                scaled[line(i, a), :] = table[at_block(q, i, a), :] * root
            scaled[line(i, i), :] = root
        for a in range(HEAD):
            own = {i: scaled[line(i, a), :] for i in range(a, HEAD)}
            for b in range(a + 1):
                total = None
                for i in range(a, HEAD):
                    term = own[i] * scaled[line(i, b), :]
                    total = term if total is None else total + term
                gap = a - b
                d, j = (gap, b) if gap <= HEAD // 2 else (HEAD - gap, a)
                forms[pl.ds((d * SPAN + j) * SUB, SUB), :] = total if gap == 0 else 2.0 * total

    def head_features(t):
        at = columns(t)
        x = effects_ref[pl.ds(0, SPAN), at]
        doubled[pl.ds(0, SPAN), :] = x
        doubled[pl.ds(HEAD, SPAN), :] = x
        j = lax.broadcasted_iota(jnp.int32, x.shape, 0)
        x = jnp.where(j < HEAD, x, 0.0)
        for d in range(LANES // SPAN):
            products[pl.ds(d * SPAN, SPAN), :] = x * doubled[pl.ds(d, SPAN), :]
        for piece, part in enumerate(split3(jnp.transpose(products[...]))[:2]):
            features[:, piece * LANES : (piece + 1) * LANES] = part

    def head_norm():
        f = [features[:, p * LANES : (p + 1) * LANES] for p in range(2)]
        w = [form_weights[pl.ds(p * LANES, LANES), :] for p in range(2)]
        left = jnp.concatenate([f[0], f[0], f[1], f[1]], axis=1)
        right = jnp.concatenate([w[0], w[1], w[0], w[1]], axis=0)
        return jnp.dot(left, right, preferred_element_type=jnp.float32)

    def prepare(t, target):
        at = columns(t)
        data = effects_ref[pl.ds(0, even), at]
        x1, x2, x3 = split3(data)
        for piece, part in enumerate((x1, x2, x1, x2, x3)):
            stack[pl.ds(piece * even, even), :] = part.astype(jnp.float32)
        for extra in range(edge_rows):
            line = effects_ref[pl.ds(even + extra, 1), at]
            x1, x2, x3 = split3(line)
            for piece, part in enumerate((x1, x2, x1, x2, x3)):
                stack[pl.ds(PIECES * even + extra * PIECES + piece, 1), :] = part.astype(jnp.float32)
        target[...] = jnp.transpose(stack[...]).astype(jnp.bfloat16)

    def conclude(t, side):
        at = columns(t)
        scores = jnp.transpose(done[...])
        top = jnp.max(scores, axis=0, keepdims=True)
        shifted = jnp.exp(scores - top)
        out_buf[side] = shifted
        peak_ref[0:1, at] = top
        peak_ref[1:2, at] = jnp.sum(shifted, axis=0, keepdims=True)

    def store(t, side):
        return pltpu.make_async_copy(out_buf.at[side], out_hbm.at[:, columns(t)], out_sem.at[side])

    def fill(batch):
        base = batch * SUB
        q = lax.rem(batch, 2)
        for s in range(SUB):
            b = slot_s[jnp.minimum(base + s, used - 1)]
            se_rows[pl.ds(s, 1), :] = se_ref[pl.ds(b, 1), :]
        ses = se_rows[...]
        squares = ses * ses
        for i in range(n):
            noise[pl.ds(i * SUB, SUB), :] = jnp.broadcast_to(squares[:, i : i + 1], (SUB, LANES))

        for rb in range(blocks):
            def fill_row(i, c):
                for j in range(rb * edge, n):
                    table[at_block(q, i, j), :] = covar_ref[pl.ds(i * rows_up + j, SUB, stride=0), :] * scale
                d = at_block(q, i, i)
                table[d, :] = table[d, :] + noise[element(i), :]
                return c

            lax.fori_loop(rb * edge, (rb + 1) * edge, fill_row, 0)

    def advance(q):
        kb = state_s[0]

        @pl.when(state_s[1] >= plan_start[kb + 1])
        def _():
            state_s[0] = kb + 1

            @pl.when(kb + 1 < blocks)
            def _():
                pivot_stage(q, kb + 1)

    def begin(q):
        state_s[0] = 0
        state_s[1] = 0
        pivot_stage(q, 0)

    def drain(q):
        def one_block(kb, c):
            position = state_s[1]

            def some(p, cc):
                for g in range(GROUP):
                    update(q, kb, plan_row[position + p * GROUP + g], plan_col[position + p * GROUP + g])
                return cc

            lax.fori_loop(0, (plan_start[kb + 1] - position) // GROUP, some, 0)
            state_s[1] = plan_start[kb + 1]

            @pl.when(kb + 1 < blocks)
            def _():
                pivot_stage(q, kb + 1)

            return c

        lax.fori_loop(state_s[0], blocks, one_block, 0)

    def one_batch(batch, carry):
        base = batch * SUB
        q = lax.rem(batch, 2)
        more = base + SUB < used

        @pl.when(batch == 0)
        def _():
            fill(batch)
            begin(q)

        drain(q)
        state_s[0] = blocks
        logs = jnp.zeros((SUB, LANES), jnp.float32)
        for i in range(n):
            d = pivots[pl.ds(i * SUB, SUB), :]
            roots[pl.ds(i * SUB, SUB), :] = lax.rsqrt(d)
            logs = logs + jnp.log(d)
        halfdet[...] = log_prior - 0.5 * logs
        head_forms(q)

        @pl.when(batch == 0)
        def _():
            fetch.wait()
            prepare(order_s[0], following)

        @pl.when(more)
        def _():
            fill(batch + 1)
            begin(1 - q)

        def one_slot(slot, c):
            s = slot - base
            for piece, part in enumerate(split3(forms[pl.ds(s, LANES, stride=SUB), :])[:2]):
                form_weights[pl.ds(piece * LANES, LANES), :] = part
            for i in range(HEAD, n):
                groups = min(i // 16 + 1, even // 16)
                rows = groups * 16
                root = roots[pl.ds(i * SUB + s, SUB, stride=0), :][0:1, :]
                row = table[pl.ds(q * (n + edge) * n * SUB + i * n * SUB + s, rows, stride=SUB), :]
                if i < even:
                    j = lax.broadcasted_iota(jnp.int32, (rows, LANES), 0)
                    row = jnp.where(j < i, row, jnp.where(j == i, 1.0, 0.0))
                row = row * root
                one = row.astype(jnp.bfloat16)
                two = (row - one.astype(jnp.float32)).astype(jnp.bfloat16)
                weights[i, pl.ds(0, rows), :] = one
                weights[i, pl.ds(even, rows), :] = two
                if i >= even:
                    first = root.astype(jnp.bfloat16)
                    second = (root - first.astype(jnp.float32)).astype(jnp.bfloat16)
                    j = lax.broadcasted_iota(jnp.int32, (16, LANES), 0)
                    tail = jnp.zeros((16, LANES), jnp.float32)
                    for piece, part in enumerate((first, first, second, second, first)):
                        tail = jnp.where(j == piece, part.astype(jnp.float32), tail)
                    weights[i, pl.ds(2 * even, 16), :] = tail.astype(jnp.bfloat16)
            row_const = halfdet[pl.ds(s, 1), :]

            def operand(i):
                one = weights[i, pl.ds(0, even), :]
                two = weights[i, pl.ds(even, even), :]
                return jnp.concatenate([one, one, two, two, one, weights[i, pl.ds(2 * even, 16), :]], axis=0)

            def one_tile(place_at, cc):
                before = order_s[jnp.maximum(place_at - 1, 0)]
                side = lax.rem(place_at, 2)

                @pl.when(place_at >= 3)
                def _():
                    store(0, 1 - side).wait()

                def body(beside):
                    flipped[...] = following[...]
                    prepare(order_s[place_at + 1], following)
                    conclude(before, 1 - side)
                    head_features(order_s[place_at])
                    for i in range(HEAD, n, 2):
                        right = jnp.concatenate([operand(r) for r in range(i, min(i + 2, n))], axis=1)
                        white = jnp.dot(flipped[...], right, preferred_element_type=jnp.float32)
                        square = white[:, :LANES] * white[:, :LANES]
                        if i + 1 < n:
                            square = square + white[:, LANES:] * white[:, LANES:]
                        if i > HEAD:
                            acc[...] += square
                        else:
                            acc[...] = square
                        if beside is not None:
                            for g in range(GROUP):
                                if (2 * g + 1) * (n - HEAD) // (2 * GROUP) // 2 == (i - HEAD) // 2:
                                    beside(g)
                    done[...] = row_const - 0.5 * (acc[...] + head_norm())

                kb = state_s[0]
                position = state_s[1]
                working = kb < blocks

                @pl.when(working)
                def _():
                    body(lambda g: update(1 - q, kb, plan_row[position + g], plan_col[position + g]))
                    state_s[1] = position + GROUP
                    advance(1 - q)

                @pl.when(jnp.logical_not(working))
                def _():
                    body(None)

                @pl.when(place_at >= 1)
                def _():
                    store(before, 1 - side).start()

                return cc

            lax.fori_loop(start_s[slot], start_s[slot + 1], one_tile, 0)
            return c

        lax.fori_loop(base, jnp.minimum(used, base + SUB), one_slot, 0)
        return carry

    lax.fori_loop(0, (used + SUB - 1) // SUB, one_batch, 0)
    last = order_s[tiles - 1]
    side = (tiles - 1) % 2
    if tiles >= 3:
        store(0, side).wait()
    conclude(last, side)
    store(last, side).start()
    if tiles >= 2:
        store(0, 1 - side).wait()
    store(last, side).wait()


def shifted_scores(effects, se_table, se_index, base_root, grid_scale, comp_base, comp_grid, weights):
    n, pairs = effects.shape
    patterns = se_table.shape[0]
    tiles = pairs // TILE
    even = n // 16 * 16
    bases = base_root.shape[0]
    rows_up = (n + SUB - 1) // SUB * SUB
    assert comp_grid.shape == (LANES,) and (n - even) * PIECES <= 16
    depth = PIECES * even + 16
    edge = block_edge(n)
    plan = update_plan(n // edge, GROUP)
    vmem = pl.BlockSpec(memory_space=pltpu.VMEM)
    smem = pl.BlockSpec(memory_space=pltpu.SMEM)
    hbm = pl.BlockSpec(memory_space=pl.ANY)
    f32 = jnp.float32
    return pl.pallas_call(
        functools.partial(main_kernel, n, tiles, patterns, grid_scale.shape[0]),
        name="shifted_scores",
        out_shape=(
            jax.ShapeDtypeStruct((LANES, pairs), f32),
            jax.ShapeDtypeStruct((2, pairs), f32),
        ),
        in_specs=[smem] * 5 + [hbm, vmem, vmem, vmem, vmem, vmem],
        out_specs=(hbm, vmem),
        scratch_shapes=[
            pltpu.VMEM((2 * (n + edge) * n * SUB, LANES), f32),
            pltpu.VMEM((n * SUB, LANES), f32),
            pltpu.VMEM(((edge * n + edge) * SUB, LANES), f32),
            pltpu.VMEM((n * SUB, LANES), f32),
            pltpu.VMEM((SUB, LANES), f32),
            pltpu.VMEM((n * SUB, LANES), f32),
            pltpu.VMEM((n, 2 * even + 16, LANES), jnp.bfloat16),
            pltpu.VMEM((n, pairs), f32),
            pltpu.VMEM((bases * rows_up, LANES), f32),
            pltpu.VMEM((n * rows_up, LANES), f32),
            pltpu.VMEM((TILE, depth), jnp.bfloat16),
            pltpu.VMEM((TILE, depth), jnp.bfloat16),
            pltpu.VMEM((depth, TILE), f32),
            pltpu.VMEM((TILE, LANES), f32),
            pltpu.VMEM((TILE, LANES), f32),
            pltpu.VMEM((2, LANES, TILE), f32),
            pltpu.VMEM((SUB, n), f32),
            pltpu.VMEM((HEAD * HEAD * SUB, LANES), f32),
            pltpu.VMEM((LANES * SUB, LANES), f32),
            pltpu.VMEM((2 * LANES, LANES), jnp.bfloat16),
            pltpu.VMEM((2 * SPAN, TILE), f32),
            pltpu.VMEM((LANES, TILE), f32),
            pltpu.VMEM((TILE, 2 * LANES), jnp.bfloat16),
            pltpu.SemaphoreType.DMA,
            pltpu.SemaphoreType.DMA((2,)),
            pltpu.SMEM((patterns + 1,), jnp.int32),
            pltpu.SMEM((patterns + 1,), jnp.int32),
            pltpu.SMEM((patterns + 1,), jnp.int32),
            pltpu.SMEM((tiles + 1,), jnp.int32),
            pltpu.SMEM((2,), jnp.int32),
        ],
        compiler_params=pltpu.CompilerParams(vmem_limit_bytes=40 * 1024 * 1024),
    )(se_index, grid_scale, *plan, effects, se_table, base_root, comp_base[None], comp_grid[None], weights[None])


def finish_kernel(width, shifted_ref, own_ref, peaks_ref, out_hbm, loglik_ref, mass_ref, buffer, sems):
    pairs = shifted_ref.shape[1]
    steps = pairs // width
    copies = []
    partial = None
    for step in range(steps):
        at = pl.ds(step * width, width)
        tops = [peaks_ref[c, 0:1, at] for c in range(peaks_ref.shape[0])]
        sums = [peaks_ref[c, 1:2, at] for c in range(peaks_ref.shape[0])]
        top = functools.reduce(jnp.maximum, tops)
        total = sum(s * jnp.exp(t - top) for s, t in zip(sums, tops))
        loglik = top + jnp.log(total)
        loglik_ref[:, at] = loglik
        factor = jnp.exp(own_ref[0:1, at] - loglik)
        for c in range(width // LANES):
            lanes = pl.ds(step * width + c * LANES, LANES)
            value = shifted_ref[:, lanes] * factor[:, c * LANES : (c + 1) * LANES]
            buffer[:, lanes] = value
            partial = value if partial is None else partial + value
        copy = pltpu.make_async_copy(buffer.at[:, at], out_hbm.at[:, at], sems.at[step])
        copy.start()
        copies.append(copy)
    mass = jnp.sum(jnp.transpose(partial), axis=0, keepdims=True)
    mass_ref[...] = jnp.broadcast_to(mass, mass_ref.shape)
    for copy in copies:
        copy.wait()


def finish(shifted, peak, peaks, receivers):
    comps, pairs = shifted.shape
    width = min(pairs, 1024)
    vmem = pl.BlockSpec(memory_space=pltpu.VMEM)
    return pl.pallas_call(
        functools.partial(finish_kernel, width),
        name="finish",
        in_specs=[vmem, vmem, vmem],
        out_specs=(pl.BlockSpec(memory_space=pl.ANY), vmem, vmem),
        out_shape=(
            jax.ShapeDtypeStruct((comps, pairs), jnp.float32),
            jax.ShapeDtypeStruct((1, pairs), jnp.float32),
            jax.ShapeDtypeStruct((receivers, comps), jnp.float32),
        ),
        scratch_shapes=[pltpu.VMEM((comps, pairs), jnp.float32), pltpu.SemaphoreType.DMA((pairs // width,))],
        compiler_params=pltpu.CompilerParams(vmem_limit_bytes=12 * 1024 * 1024),
    )(shifted, peak, peaks)


def per_device(effects, se_table, se_index, base_root, grid_scale, comp_base, comp_grid, weights):
    n, pairs = effects.shape
    comps = comp_base.shape[0]
    shifted, peak = shifted_scores(effects, se_table, se_index, base_root, grid_scale, comp_base, comp_grid, weights)
    peaks = lax.all_gather(peak, "comp")
    receivers = lax.axis_size("pairs")
    responsibility, loglik, mass = finish(shifted, peak, peaks, receivers)
    masses = jnp.sum(lax.all_to_all(mass, "pairs", 0, 0, tiled=True), axis=0)
    all_pairs = pairs * lax.axis_size("pairs")
    all_comps = comps * lax.axis_size("comp")
    log_weights = jnp.log((masses + 1.0) / (all_pairs + all_comps))
    return (responsibility, log_weights, loglik[0])


def solution(mesh):
    placed = (P(None, "pairs"), P(), P("pairs"), P(), P(), P("comp"), P("comp"), P("comp"))
    return jax.shard_map(
        per_device,
        mesh=mesh,
        in_specs=placed,
        out_specs=(P("comp", "pairs"), P("comp"), P("pairs")),
        check_vma=False,
    )
```

```python
import functools
import math

import jax
import jax.numpy as jnp
import numpy as np
from jax import lax
from jax.experimental import pallas as pl
from jax.experimental.pallas import tpu as pltpu
from jax.sharding import PartitionSpec as P

TILE = 512
SUB = 8
LANES = 128
PIECES = 5
GROUP = 5
ROWS = 3
HEAD = 15
SPAN = 16


def block_edge(count):
    return max(edge for edge in range(1, 9) if count % edge == 0)


def element(index):
    return pl.ds(pl.multiple_of(index * SUB, SUB), SUB)


def update_plan(blocks, group):
    lists = []
    for kb in range(blocks):
        pairs = [(ib, jb) for ib in range(kb + 1, blocks) for jb in list(range(kb)) + list(range(ib + 1, blocks))]
        while len(pairs) % group:
            pairs.append((blocks, 0))
        lists.append(pairs)
    flat = [pair for pairs in lists for pair in pairs]
    starts = np.cumsum([0] + [len(pairs) for pairs in lists])
    return tuple(np.array(a, np.int32) for a in ([p[0] for p in flat], [p[1] for p in flat], starts))


def elimination(n, table, pivots, factors):
    edge = block_edge(n)
    blocks = n // edge

    def at(q, i, j):
        return element(q * (n + edge) * n + i * n + j)

    def pivot_stage(q, kb):
        first = kb * edge
        diag = [[table[at(q, first + m, first + j), :] if j >= m else None for j in range(edge)] for m in range(edge)]
        lower = [[None] * edge for _ in range(edge)]
        inverse = [[None] * edge for _ in range(edge)]
        recips = []
        for m in range(edge):
            d = diag[m][m]
            recip = 1.0 / d
            recips.append(recip)
            pivots[element(first + m), :] = d
            for r in range(m + 1, edge):
                lower[r][m] = diag[m][r] * recip
            for r in range(m + 1, edge):
                for j in range(r, edge):
                    diag[r][j] = diag[r][j] - lower[r][m] * diag[m][j]
                for j in range(m):
                    inverse[r][j] = inverse[r][j] - lower[r][m] * inverse[m][j]
                inverse[r][m] = -lower[r][m]
        for r in range(edge):
            for j in range(r):
                table[at(q, first + r, first + j), :] = inverse[r][j]

        def column_block(jb, with_factor):
            col = jb * edge
            for j in range(edge):
                rows = [table[at(q, first + m, col + j), :] for m in range(edge)]
                for m in range(edge):
                    for r in range(m + 1, edge):
                        rows[r] = rows[r] - lower[r][m] * rows[m]
                for m in range(edge):
                    if m:
                        table[at(q, first + m, col + j), :] = rows[m]
                    if with_factor:
                        factors[element(m * n + col + j), :] = rows[m] * recips[m]

        def left(jb, c):
            column_block(jb, False)
            return c

        def right(jb, c):
            column_block(jb, True)
            return c

        lax.fori_loop(0, kb, left, 0)
        lax.fori_loop(kb + 1, blocks, right, 0)

        def row_block(ib, c):
            row = ib * edge
            for start in range(0, edge, ROWS):
                rows = range(start, min(start + ROWS, edge))
                size = len(rows)
                f = [[factors[element(m * n + row + i), :] for m in range(edge)] for i in rows]
                totals = [list(line) for line in f]
                for m in range(1, edge):
                    for j in range(m):
                        v = table[at(q, first + m, first + j), :]
                        for a in range(size):
                            totals[a][j] = totals[a][j] + f[a][m] * v
                values = {}
                for j in range(rows[0], edge):
                    live = [a for a, i in enumerate(rows) if i <= j]
                    for a in live:
                        values[a, j] = table[at(q, row + rows[a], row + j), :]
                    for m in range(edge):
                        u = table[at(q, first + m, row + j), :]
                        for a in live:
                            values[a, j] = values[a, j] - f[a][m] * u
                for a, i in enumerate(rows):
                    for j in range(edge):
                        table[at(q, row + i, first + j), :] = -totals[a][j]
                for (a, j), v in values.items():
                    table[at(q, row + rows[a], row + j), :] = v

            return c

        lax.fori_loop(kb + 1, blocks, row_block, 0)

    def update(q, kb, ib, jb):
        first, row, col = kb * edge, ib * edge, jb * edge
        start = 0
        for size in (edge - edge // 2, edge // 2):
            rows = range(start, start + size)
            start += size
            held = [[table[at(q, row + i, col + j), :] for j in range(edge)] for i in rows]
            for m in range(edge):
                f = [factors[element(m * n + row + i), :] for i in rows]
                for j in range(edge):
                    u = table[at(q, first + m, col + j), :]
                    for a in range(len(f)):
                        held[a][j] = held[a][j] - f[a] * u
            for a, i in enumerate(rows):
                for j in range(edge):
                    table[at(q, row + i, col + j), :] = held[a][j]

    return at, pivot_stage, update


def split3(value):
    one = value.astype(jnp.bfloat16)
    rest = value - one.astype(jnp.float32)
    two = rest.astype(jnp.bfloat16)
    three = (rest - two.astype(jnp.float32)).astype(jnp.bfloat16)
    return one, two, three


def main_kernel(
    n, tiles, patterns, grids,
    index_ref, grid_ref, plan_row, plan_col, plan_start, effects_hbm, se_ref, covar_hbm, comp_grid_ref, prior_ref,
    out_hbm, peak_ref,
    table, pivots, factors, roots, halfdet, noise, weights, effects_ref, covar_ref, flipped, following, stack, acc, done, out_buf, se_rows,
    scaled, forms, form_weights, doubled, products, features,
    in_sem, covar_sem, out_sem,
    count_s, start_s, slot_s, order_s, state_s,
):
    even = n // 16 * 16
    edge_rows = n - even
    edge = block_edge(n)
    blocks = n // edge
    at_block, pivot_stage, update = elimination(n, table, pivots, factors)
    fetch = pltpu.make_async_copy(effects_hbm, effects_ref, in_sem)
    fetch.start()
    fetch_covar = pltpu.make_async_copy(covar_hbm, covar_ref, covar_sem)
    fetch_covar.start()

    def clear(b, c):
        count_s[b] = 0
        return c

    lax.fori_loop(0, patterns, clear, 0)

    def tally(t, c):
        b = index_ref[t]
        count_s[b] = count_s[b] + 1
        return c

    lax.fori_loop(0, tiles, tally, 0)

    def place(b, state):
        used, offset = state
        many = count_s[b]
        slot_s[used] = b
        start_s[used] = offset
        count_s[b] = offset
        return used + jnp.where(many > 0, 1, 0), offset + many

    used, _ = lax.fori_loop(0, patterns, place, (jnp.int32(0), jnp.int32(0)))
    start_s[used] = tiles

    def sort(t, c):
        b = index_ref[t]
        position = count_s[b]
        order_s[position] = t
        count_s[b] = position + 1
        return c

    lax.fori_loop(0, tiles, sort, 0)
    order_s[tiles] = 0

    weights[...] = jnp.zeros_like(weights)
    stack[...] = jnp.zeros_like(stack)
    forms[...] = jnp.zeros_like(forms)
    doubled[...] = jnp.zeros_like(doubled)
    chosen = comp_grid_ref[...]
    scale = jnp.zeros(chosen.shape, jnp.float32)
    for g in range(grids):
        scale = jnp.where(chosen == g, grid_ref[g], scale)
    scale = jnp.broadcast_to(scale * scale, (SUB, LANES))
    log_prior = jnp.log(prior_ref[...]) - 0.5 * n * math.log(2.0 * math.pi)

    fetch_covar.wait()

    def columns(t):
        return pl.ds(pl.multiple_of(t * TILE, TILE), TILE)

    def head_forms(q):
        def line(i, a):
            return pl.ds((i * HEAD + a) * SUB, SUB)

        for i in range(HEAD):
            root = roots[pl.ds(i * SUB, SUB), :]
            for a in range(i):
                scaled[line(i, a), :] = table[at_block(q, i, a), :] * root
            scaled[line(i, i), :] = root
        for a in range(HEAD):
            own = {i: scaled[line(i, a), :] for i in range(a, HEAD)}
            for b in range(a + 1):
                total = None
                for i in range(a, HEAD):
                    term = own[i] * scaled[line(i, b), :]
                    total = term if total is None else total + term
                gap = a - b
                d, j = (gap, b) if gap <= HEAD // 2 else (HEAD - gap, a)
                forms[pl.ds((d * SPAN + j) * SUB, SUB), :] = total if gap == 0 else 2.0 * total

    def head_features(t):
        at = columns(t)
        x = effects_ref[pl.ds(0, SPAN), at]
        doubled[pl.ds(0, SPAN), :] = x
        doubled[pl.ds(HEAD, SPAN), :] = x
        j = lax.broadcasted_iota(jnp.int32, x.shape, 0)
        x = jnp.where(j < HEAD, x, 0.0)
        for d in range(LANES // SPAN):
            products[pl.ds(d * SPAN, SPAN), :] = x * doubled[pl.ds(d, SPAN), :]
        for piece, part in enumerate(split3(jnp.transpose(products[...]))[:2]):
            features[:, piece * LANES : (piece + 1) * LANES] = part

    def head_norm():
        f = [features[:, p * LANES : (p + 1) * LANES] for p in range(2)]
        w = [form_weights[pl.ds(p * LANES, LANES), :] for p in range(2)]
        left = jnp.concatenate([f[0], f[0], f[1], f[1]], axis=1)
        right = jnp.concatenate([w[0], w[1], w[0], w[1]], axis=0)
        return jnp.dot(left, right, preferred_element_type=jnp.float32)

    def prepare(t, target):
        at = columns(t)
        data = effects_ref[pl.ds(0, even), at]
        x1, x2, x3 = split3(data)
        for piece, part in enumerate((x1, x2, x1, x2, x3)):
            stack[pl.ds(piece * even, even), :] = part.astype(jnp.float32)
        for extra in range(edge_rows):
            line = effects_ref[pl.ds(even + extra, 1), at]
            x1, x2, x3 = split3(line)
            for piece, part in enumerate((x1, x2, x1, x2, x3)):
                stack[pl.ds(PIECES * even + extra * PIECES + piece, 1), :] = part.astype(jnp.float32)
        target[...] = jnp.transpose(stack[...]).astype(jnp.bfloat16)

    def conclude(t, side):
        at = columns(t)
        scores = jnp.transpose(done[...])
        top = jnp.max(scores, axis=0, keepdims=True)
        shifted = jnp.exp(scores - top)
        out_buf[side] = shifted
        peak_ref[0:1, at] = top
        peak_ref[1:2, at] = jnp.sum(shifted, axis=0, keepdims=True)

    def store(t, side):
        return pltpu.make_async_copy(out_buf.at[side], out_hbm.at[:, columns(t)], out_sem.at[side])

    def fill(batch):
        base = batch * SUB
        q = lax.rem(batch, 2)
        for s in range(SUB):
            b = slot_s[jnp.minimum(base + s, used - 1)]
            se_rows[pl.ds(s, 1), :] = se_ref[pl.ds(b, 1), :]
        ses = se_rows[...]
        squares = ses * ses
        for i in range(n):
            noise[pl.ds(i * SUB, SUB), :] = jnp.broadcast_to(squares[:, i : i + 1], (SUB, LANES))

        for rb in range(blocks):
            def fill_row(i, c):
                for j in range(rb * edge, n):
                    table[at_block(q, i, j), :] = covar_ref[pl.ds(i * n + j, SUB, stride=0), :] * scale
                d = at_block(q, i, i)
                table[d, :] = table[d, :] + noise[element(i), :]
                return c

            lax.fori_loop(rb * edge, (rb + 1) * edge, fill_row, 0)

    def advance(q):
        kb = state_s[0]

        @pl.when(state_s[1] >= plan_start[kb + 1])
        def _():
            state_s[0] = kb + 1

            @pl.when(kb + 1 < blocks)
            def _():
                pivot_stage(q, kb + 1)

    def begin(q):
        state_s[0] = 0
        state_s[1] = 0
        pivot_stage(q, 0)

    def drain(q):
        def one_block(kb, c):
            position = state_s[1]

            def some(p, cc):
                for g in range(GROUP):
                    update(q, kb, plan_row[position + p * GROUP + g], plan_col[position + p * GROUP + g])
                return cc

            lax.fori_loop(0, (plan_start[kb + 1] - position) // GROUP, some, 0)
            state_s[1] = plan_start[kb + 1]

            @pl.when(kb + 1 < blocks)
            def _():
                pivot_stage(q, kb + 1)

            return c

        lax.fori_loop(state_s[0], blocks, one_block, 0)

    def one_batch(batch, carry):
        base = batch * SUB
        q = lax.rem(batch, 2)
        more = base + SUB < used

        @pl.when(batch == 0)
        def _():
            fill(batch)
            begin(q)

        drain(q)
        state_s[0] = blocks
        logs = jnp.zeros((SUB, LANES), jnp.float32)
        for i in range(n):
            d = pivots[pl.ds(i * SUB, SUB), :]
            roots[pl.ds(i * SUB, SUB), :] = lax.rsqrt(d)
            logs = logs + jnp.log(d)
        halfdet[...] = log_prior - 0.5 * logs
        head_forms(q)

        @pl.when(batch == 0)
        def _():
            fetch.wait()
            prepare(order_s[0], following)

        @pl.when(more)
        def _():
            fill(batch + 1)
            begin(1 - q)

        def one_slot(slot, c):
            s = slot - base
            for piece, part in enumerate(split3(forms[pl.ds(s, LANES, stride=SUB), :])[:2]):
                form_weights[pl.ds(piece * LANES, LANES), :] = part
            for i in range(HEAD, n):
                groups = min(i // 16 + 1, even // 16)
                rows = groups * 16
                root = roots[pl.ds(i * SUB + s, SUB, stride=0), :][0:1, :]
                row = table[pl.ds(q * (n + edge) * n * SUB + i * n * SUB + s, rows, stride=SUB), :]
                if i < even:
                    j = lax.broadcasted_iota(jnp.int32, (rows, LANES), 0)
                    row = jnp.where(j < i, row, jnp.where(j == i, 1.0, 0.0))
                row = row * root
                one = row.astype(jnp.bfloat16)
                two = (row - one.astype(jnp.float32)).astype(jnp.bfloat16)
                weights[i, pl.ds(0, rows), :] = one
                weights[i, pl.ds(even, rows), :] = two
                if i >= even:
                    first = root.astype(jnp.bfloat16)
                    second = (root - first.astype(jnp.float32)).astype(jnp.bfloat16)
                    j = lax.broadcasted_iota(jnp.int32, (16, LANES), 0)
                    tail = jnp.zeros((16, LANES), jnp.float32)
                    for piece, part in enumerate((first, first, second, second, first)):
                        tail = jnp.where(j == piece, part.astype(jnp.float32), tail)
                    weights[i, pl.ds(2 * even, 16), :] = tail.astype(jnp.bfloat16)
            row_const = halfdet[pl.ds(s, 1), :]

            def operand(i):
                one = weights[i, pl.ds(0, even), :]
                two = weights[i, pl.ds(even, even), :]
                return jnp.concatenate([one, one, two, two, one, weights[i, pl.ds(2 * even, 16), :]], axis=0)

            def one_tile(place_at, cc):
                before = order_s[jnp.maximum(place_at - 1, 0)]
                side = lax.rem(place_at, 2)

                @pl.when(place_at >= 3)
                def _():
                    store(0, 1 - side).wait()

                def body(beside):
                    flipped[...] = following[...]
                    prepare(order_s[place_at + 1], following)
                    conclude(before, 1 - side)
                    head_features(order_s[place_at])
                    for i in range(HEAD, n, 2):
                        right = jnp.concatenate([operand(r) for r in range(i, min(i + 2, n))], axis=1)
                        white = jnp.dot(flipped[...], right, preferred_element_type=jnp.float32)
                        square = white[:, :LANES] * white[:, :LANES]
                        if i + 1 < n:
                            square = square + white[:, LANES:] * white[:, LANES:]
                        if i > HEAD:
                            acc[...] += square
                        else:
                            acc[...] = square
                        if beside is not None:
                            for g in range(GROUP):
                                if (2 * g + 1) * (n - HEAD) // (2 * GROUP) // 2 == (i - HEAD) // 2:
                                    beside(g)
                    done[...] = row_const - 0.5 * (acc[...] + head_norm())

                kb = state_s[0]
                position = state_s[1]
                working = kb < blocks

                @pl.when(working)
                def _():
                    body(lambda g: update(1 - q, kb, plan_row[position + g], plan_col[position + g]))
                    state_s[1] = position + GROUP
                    advance(1 - q)

                @pl.when(jnp.logical_not(working))
                def _():
                    body(None)

                @pl.when(place_at >= 1)
                def _():
                    store(before, 1 - side).start()

                return cc

            lax.fori_loop(start_s[slot], start_s[slot + 1], one_tile, 0)
            return c

        lax.fori_loop(base, jnp.minimum(used, base + SUB), one_slot, 0)
        return carry

    lax.fori_loop(0, (used + SUB - 1) // SUB, one_batch, 0)
    last = order_s[tiles - 1]
    side = (tiles - 1) % 2
    if tiles >= 3:
        store(0, side).wait()
    conclude(last, side)
    store(last, side).start()
    if tiles >= 2:
        store(0, 1 - side).wait()
    store(last, side).wait()


def shifted_scores(effects, se_table, se_index, covar, grid_scale, comp_grid, weights):
    n, pairs = effects.shape
    patterns = se_table.shape[0]
    tiles = pairs // TILE
    even = n // 16 * 16
    assert covar.shape == (n * n, LANES) and (n - even) * PIECES <= 16
    depth = PIECES * even + 16
    edge = block_edge(n)
    plan = update_plan(n // edge, GROUP)
    vmem = pl.BlockSpec(memory_space=pltpu.VMEM)
    smem = pl.BlockSpec(memory_space=pltpu.SMEM)
    hbm = pl.BlockSpec(memory_space=pl.ANY)
    f32 = jnp.float32
    return pl.pallas_call(
        functools.partial(main_kernel, n, tiles, patterns, grid_scale.shape[0]),
        name="shifted_scores",
        out_shape=(
            jax.ShapeDtypeStruct((LANES, pairs), f32),
            jax.ShapeDtypeStruct((2, pairs), f32),
        ),
        in_specs=[smem] * 5 + [hbm, vmem, hbm, vmem, vmem],
        out_specs=(hbm, vmem),
        scratch_shapes=[
            pltpu.VMEM((2 * (n + edge) * n * SUB, LANES), f32),
            pltpu.VMEM((n * SUB, LANES), f32),
            pltpu.VMEM(((edge * n + edge) * SUB, LANES), f32),
            pltpu.VMEM((n * SUB, LANES), f32),
            pltpu.VMEM((SUB, LANES), f32),
            pltpu.VMEM((n * SUB, LANES), f32),
            pltpu.VMEM((n, 2 * even + 16, LANES), jnp.bfloat16),
            pltpu.VMEM((n, pairs), f32),
            pltpu.VMEM((n * n, LANES), f32),
            pltpu.VMEM((TILE, depth), jnp.bfloat16),
            pltpu.VMEM((TILE, depth), jnp.bfloat16),
            pltpu.VMEM((depth, TILE), f32),
            pltpu.VMEM((TILE, LANES), f32),
            pltpu.VMEM((TILE, LANES), f32),
            pltpu.VMEM((2, LANES, TILE), f32),
            pltpu.VMEM((SUB, n), f32),
            pltpu.VMEM((HEAD * HEAD * SUB, LANES), f32),
            pltpu.VMEM((LANES * SUB, LANES), f32),
            pltpu.VMEM((2 * LANES, LANES), jnp.bfloat16),
            pltpu.VMEM((2 * SPAN, TILE), f32),
            pltpu.VMEM((LANES, TILE), f32),
            pltpu.VMEM((TILE, 2 * LANES), jnp.bfloat16),
            pltpu.SemaphoreType.DMA,
            pltpu.SemaphoreType.DMA,
            pltpu.SemaphoreType.DMA((2,)),
            pltpu.SMEM((patterns + 1,), jnp.int32),
            pltpu.SMEM((patterns + 1,), jnp.int32),
            pltpu.SMEM((patterns + 1,), jnp.int32),
            pltpu.SMEM((tiles + 1,), jnp.int32),
            pltpu.SMEM((2,), jnp.int32),
        ],
        compiler_params=pltpu.CompilerParams(vmem_limit_bytes=40 * 1024 * 1024),
    )(se_index, grid_scale, *plan, effects, se_table, covar, comp_grid[None], weights[None])


def exact_dot(left, right, dims):
    return lax.dot_general(left, right, (dims, ((), ())), precision=lax.Precision.HIGHEST, preferred_element_type=jnp.float32)


def finish_kernel(width, shifted_ref, own_ref, peaks_ref, out_hbm, loglik_ref, mass_ref, buffer, sems):
    pairs = shifted_ref.shape[1]
    steps = pairs // width
    copies = []
    partial = None
    for step in range(steps):
        at = pl.ds(step * width, width)
        tops = [peaks_ref[c, 0:1, at] for c in range(peaks_ref.shape[0])]
        sums = [peaks_ref[c, 1:2, at] for c in range(peaks_ref.shape[0])]
        top = functools.reduce(jnp.maximum, tops)
        total = sum(s * jnp.exp(t - top) for s, t in zip(sums, tops))
        loglik = top + jnp.log(total)
        loglik_ref[:, at] = loglik
        factor = jnp.exp(own_ref[0:1, at] - loglik)
        for c in range(width // LANES):
            lanes = pl.ds(step * width + c * LANES, LANES)
            value = shifted_ref[:, lanes] * factor[:, c * LANES : (c + 1) * LANES]
            buffer[:, lanes] = value
            partial = value if partial is None else partial + value
        copy = pltpu.make_async_copy(buffer.at[:, at], out_hbm.at[:, at], sems.at[step])
        copy.start()
        copies.append(copy)
    mass = jnp.sum(jnp.transpose(partial), axis=0, keepdims=True)
    mass_ref[...] = jnp.broadcast_to(mass, mass_ref.shape)
    for copy in copies:
        copy.wait()


def finish(shifted, peak, peaks, receivers):
    comps, pairs = shifted.shape
    width = min(pairs, 1024)
    vmem = pl.BlockSpec(memory_space=pltpu.VMEM)
    return pl.pallas_call(
        functools.partial(finish_kernel, width),
        name="finish",
        in_specs=[vmem, vmem, vmem],
        out_specs=(pl.BlockSpec(memory_space=pl.ANY), vmem, vmem),
        out_shape=(
            jax.ShapeDtypeStruct((comps, pairs), jnp.float32),
            jax.ShapeDtypeStruct((1, pairs), jnp.float32),
            jax.ShapeDtypeStruct((receivers, comps), jnp.float32),
        ),
        scratch_shapes=[pltpu.VMEM((comps, pairs), jnp.float32), pltpu.SemaphoreType.DMA((pairs // width,))],
        compiler_params=pltpu.CompilerParams(vmem_limit_bytes=12 * 1024 * 1024),
    )(shifted, peak, peaks)


def per_device(effects, se_table, se_index, base_root, grid_scale, comp_base, comp_grid, weights):
    n, pairs = effects.shape
    comps = comp_base.shape[0]
    covariances = jnp.einsum("uij,ukj->uik", base_root, base_root, precision=lax.Precision.HIGHEST)
    covariances = covariances.reshape(covariances.shape[0], n * n)
    bases = jnp.arange(covariances.shape[0], dtype=jnp.int32)
    pick = (comp_base[None] == bases[:, None]).astype(jnp.float32)
    covar = exact_dot(covariances, pick, ((0,), (0,)))
    shifted, peak = shifted_scores(effects, se_table, se_index, covar, grid_scale, comp_grid, weights)
    peaks = lax.all_gather(peak, "comp")
    receivers = lax.axis_size("pairs")
    responsibility, loglik, mass = finish(shifted, peak, peaks, receivers)
    masses = jnp.sum(lax.all_to_all(mass, "pairs", 0, 0, tiled=True), axis=0)
    all_pairs = pairs * lax.axis_size("pairs")
    all_comps = comps * lax.axis_size("comp")
    log_weights = jnp.log((masses + 1.0) / (all_pairs + all_comps))
    return (responsibility, log_weights, loglik[0])


def solution(mesh):
    placed = (P(None, "pairs"), P(), P("pairs"), P(), P(), P("comp"), P("comp"), P("comp"))
    return jax.shard_map(
        per_device,
        mesh=mesh,
        in_specs=placed,
        out_specs=(P("comp", "pairs"), P("comp"), P("pairs")),
        check_vma=False,
    )
```

```python
import functools
import math

import jax
import jax.numpy as jnp
import numpy as np
from jax import lax
from jax.experimental import pallas as pl
from jax.experimental.pallas import tpu as pltpu
from jax.sharding import PartitionSpec as P

TILE = 512
SUB = 8
LANES = 128
PIECES = 5
GROUP = 5
ROWS = 3
HEAD = 15
SPAN = 16


def block_edge(count):
    return max(edge for edge in range(1, 9) if count % edge == 0)


def element(index):
    return pl.ds(pl.multiple_of(index * SUB, SUB), SUB)


def update_plan(blocks, group):
    lists = []
    for kb in range(blocks):
        pairs = [(ib, jb) for ib in range(kb + 1, blocks) for jb in list(range(kb)) + list(range(ib + 1, blocks))]
        while len(pairs) % group:
            pairs.append((blocks, 0))
        lists.append(pairs)
    flat = [pair for pairs in lists for pair in pairs]
    starts = np.cumsum([0] + [len(pairs) for pairs in lists])
    return tuple(np.array(a, np.int32) for a in ([p[0] for p in flat], [p[1] for p in flat], starts))


def elimination(n, table, pivots, factors):
    edge = block_edge(n)
    blocks = n // edge

    def at(q, i, j):
        return element(q * (n + edge) * n + i * n + j)

    def pivot_stage(q, kb):
        first = kb * edge
        diag = [[table[at(q, first + m, first + j), :] if j >= m else None for j in range(edge)] for m in range(edge)]
        lower = [[None] * edge for _ in range(edge)]
        inverse = [[None] * edge for _ in range(edge)]
        recips = []
        for m in range(edge):
            d = diag[m][m]
            recip = 1.0 / d
            recips.append(recip)
            pivots[element(first + m), :] = d
            for r in range(m + 1, edge):
                lower[r][m] = diag[m][r] * recip
            for r in range(m + 1, edge):
                for j in range(r, edge):
                    diag[r][j] = diag[r][j] - lower[r][m] * diag[m][j]
                for j in range(m):
                    inverse[r][j] = inverse[r][j] - lower[r][m] * inverse[m][j]
                inverse[r][m] = -lower[r][m]
        for r in range(edge):
            for j in range(r):
                table[at(q, first + r, first + j), :] = inverse[r][j]

        def column_block(jb, with_factor):
            col = jb * edge
            for j in range(edge):
                rows = [table[at(q, first + m, col + j), :] for m in range(edge)]
                for m in range(edge):
                    for r in range(m + 1, edge):
                        rows[r] = rows[r] - lower[r][m] * rows[m]
                for m in range(edge):
                    if m:
                        table[at(q, first + m, col + j), :] = rows[m]
                    if with_factor:
                        factors[element(m * n + col + j), :] = rows[m] * recips[m]

        def left(jb, c):
            column_block(jb, False)
            return c

        def right(jb, c):
            column_block(jb, True)
            return c

        lax.fori_loop(0, kb, left, 0)
        lax.fori_loop(kb + 1, blocks, right, 0)

        def row_block(ib, c):
            row = ib * edge
            for start in range(0, edge, ROWS):
                rows = range(start, min(start + ROWS, edge))
                size = len(rows)
                f = [[factors[element(m * n + row + i), :] for m in range(edge)] for i in rows]
                totals = [list(line) for line in f]
                for m in range(1, edge):
                    for j in range(m):
                        v = table[at(q, first + m, first + j), :]
                        for a in range(size):
                            totals[a][j] = totals[a][j] + f[a][m] * v
                values = {}
                for j in range(rows[0], edge):
                    live = [a for a, i in enumerate(rows) if i <= j]
                    for a in live:
                        values[a, j] = table[at(q, row + rows[a], row + j), :]
                    for m in range(edge):
                        u = table[at(q, first + m, row + j), :]
                        for a in live:
                            values[a, j] = values[a, j] - f[a][m] * u
                for a, i in enumerate(rows):
                    for j in range(edge):
                        table[at(q, row + i, first + j), :] = -totals[a][j]
                for (a, j), v in values.items():
                    table[at(q, row + rows[a], row + j), :] = v

            return c

        lax.fori_loop(kb + 1, blocks, row_block, 0)

    def update(q, kb, ib, jb):
        first, row, col = kb * edge, ib * edge, jb * edge
        start = 0
        for size in (edge - edge // 2, edge // 2):
            rows = range(start, start + size)
            start += size
            held = [[table[at(q, row + i, col + j), :] for j in range(edge)] for i in rows]
            for m in range(edge):
                f = [factors[element(m * n + row + i), :] for i in rows]
                for j in range(edge):
                    u = table[at(q, first + m, col + j), :]
                    for a in range(len(f)):
                        held[a][j] = held[a][j] - f[a] * u
            for a, i in enumerate(rows):
                for j in range(edge):
                    table[at(q, row + i, col + j), :] = held[a][j]

    return at, pivot_stage, update


def split3(value):
    one = value.astype(jnp.bfloat16)
    rest = value - one.astype(jnp.float32)
    two = rest.astype(jnp.bfloat16)
    three = (rest - two.astype(jnp.float32)).astype(jnp.bfloat16)
    return one, two, three


def main_kernel(
    n, tiles, patterns, grids,
    index_ref, grid_ref, plan_row, plan_col, plan_start, effects_hbm, se_ref, covar_hbm, comp_grid_ref, prior_ref,
    out_hbm, peak_ref,
    table, pivots, factors, roots, halfdet, noise, weights, effects_ref, covar_ref, flipped, following, stack, acc, done, out_buf, se_rows,
    scaled, forms, form_weights, doubled, products, features,
    in_sem, covar_sem, out_sem,
    count_s, start_s, slot_s, order_s, state_s,
):
    even = n // 16 * 16
    edge_rows = n - even
    edge = block_edge(n)
    blocks = n // edge
    at_block, pivot_stage, update = elimination(n, table, pivots, factors)
    fetch = pltpu.make_async_copy(effects_hbm, effects_ref, in_sem)
    fetch.start()
    fetch_covar = pltpu.make_async_copy(covar_hbm, covar_ref, covar_sem)
    fetch_covar.start()

    def clear(b, c):
        count_s[b] = 0
        return c

    lax.fori_loop(0, patterns, clear, 0)

    def tally(t, c):
        b = index_ref[t]
        count_s[b] = count_s[b] + 1
        return c

    lax.fori_loop(0, tiles, tally, 0)

    def place(least, most):
        def one(b, state):
            used, offset = state
            many = count_s[b]
            take = jnp.logical_and(many >= least, many <= most)

            @pl.when(take)
            def _():
                slot_s[used] = b
                start_s[used] = offset
                count_s[b] = offset + tiles + 1

            return used + jnp.where(take, 1, 0), offset + jnp.where(take, many, 0)

        return one

    found = lax.fori_loop(0, patterns, place(2, tiles), (jnp.int32(0), jnp.int32(0)))
    used, _ = lax.fori_loop(0, patterns, place(1, 1), found)
    start_s[used] = tiles

    def sort(t, c):
        b = index_ref[t]
        position = count_s[b]
        order_s[position - tiles - 1] = t
        count_s[b] = position + 1
        return c

    lax.fori_loop(0, tiles, sort, 0)
    order_s[tiles] = 0

    weights[...] = jnp.zeros_like(weights)
    stack[...] = jnp.zeros_like(stack)
    forms[...] = jnp.zeros_like(forms)
    doubled[...] = jnp.zeros_like(doubled)
    chosen = comp_grid_ref[...]
    scale = jnp.zeros(chosen.shape, jnp.float32)
    for g in range(grids):
        scale = jnp.where(chosen == g, grid_ref[g], scale)
    scale = jnp.broadcast_to(scale * scale, (SUB, LANES))
    log_prior = jnp.log(prior_ref[...]) - 0.5 * n * math.log(2.0 * math.pi)

    fetch_covar.wait()

    def columns(t):
        return pl.ds(pl.multiple_of(t * TILE, TILE), TILE)

    def head_forms(q):
        def line(i, a):
            return pl.ds((i * HEAD + a) * SUB, SUB)

        for i in range(HEAD):
            root = roots[pl.ds(i * SUB, SUB), :]
            for a in range(i):
                scaled[line(i, a), :] = table[at_block(q, i, a), :] * root
            scaled[line(i, i), :] = root
        for a in range(HEAD):
            own = {i: scaled[line(i, a), :] for i in range(a, HEAD)}
            for b in range(a + 1):
                total = None
                for i in range(a, HEAD):
                    term = own[i] * scaled[line(i, b), :]
                    total = term if total is None else total + term
                gap = a - b
                d, j = (gap, b) if gap <= HEAD // 2 else (HEAD - gap, a)
                forms[pl.ds((d * SPAN + j) * SUB, SUB), :] = total if gap == 0 else 2.0 * total

    def head_features(t):
        at = columns(t)
        x = effects_ref[pl.ds(0, SPAN), at]
        doubled[pl.ds(0, SPAN), :] = x
        doubled[pl.ds(HEAD, SPAN), :] = x
        j = lax.broadcasted_iota(jnp.int32, x.shape, 0)
        x = jnp.where(j < HEAD, x, 0.0)
        for d in range(LANES // SPAN):
            products[pl.ds(d * SPAN, SPAN), :] = x * doubled[pl.ds(d, SPAN), :]
        for piece, part in enumerate(split3(jnp.transpose(products[...]))[:2]):
            features[:, piece * LANES : (piece + 1) * LANES] = part

    def head_norm():
        f = [features[:, p * LANES : (p + 1) * LANES] for p in range(2)]
        w = [form_weights[pl.ds(p * LANES, LANES), :] for p in range(2)]
        left = jnp.concatenate([f[0], f[0], f[1], f[1]], axis=1)
        right = jnp.concatenate([w[0], w[1], w[0], w[1]], axis=0)
        return jnp.dot(left, right, preferred_element_type=jnp.float32)

    def prepare(t, target):
        at = columns(t)
        data = effects_ref[pl.ds(0, even), at]
        x1, x2, x3 = split3(data)
        for piece, part in enumerate((x1, x2, x1, x2, x3)):
            stack[pl.ds(piece * even, even), :] = part.astype(jnp.float32)
        for extra in range(edge_rows):
            line = effects_ref[pl.ds(even + extra, 1), at]
            x1, x2, x3 = split3(line)
            for piece, part in enumerate((x1, x2, x1, x2, x3)):
                stack[pl.ds(PIECES * even + extra * PIECES + piece, 1), :] = part.astype(jnp.float32)
        target[...] = jnp.transpose(stack[...]).astype(jnp.bfloat16)

    def conclude(t, side):
        at = columns(t)
        scores = jnp.transpose(done[...])
        top = jnp.max(scores, axis=0, keepdims=True)
        shifted = jnp.exp(scores - top)
        out_buf[side] = shifted
        peak_ref[0:1, at] = top
        peak_ref[1:2, at] = jnp.sum(shifted, axis=0, keepdims=True)

    def store(t, side):
        return pltpu.make_async_copy(out_buf.at[side], out_hbm.at[:, columns(t)], out_sem.at[side])

    def fill(batch):
        base = batch * SUB
        q = lax.rem(batch, 2)
        for s in range(SUB):
            b = slot_s[jnp.minimum(base + s, used - 1)]
            se_rows[pl.ds(s, 1), :] = se_ref[pl.ds(b, 1), :]
        ses = se_rows[...]
        squares = ses * ses
        for i in range(n):
            noise[pl.ds(i * SUB, SUB), :] = jnp.broadcast_to(squares[:, i : i + 1], (SUB, LANES))

        for rb in range(blocks):
            def fill_row(i, c):
                for j in range(rb * edge, n):
                    table[at_block(q, i, j), :] = covar_ref[pl.ds(i * n + j, SUB, stride=0), :] * scale
                d = at_block(q, i, i)
                table[d, :] = table[d, :] + noise[element(i), :]
                return c

            lax.fori_loop(rb * edge, (rb + 1) * edge, fill_row, 0)

    def advance(q):
        kb = state_s[0]

        @pl.when(state_s[1] >= plan_start[kb + 1])
        def _():
            state_s[0] = kb + 1

            @pl.when(kb + 1 < blocks)
            def _():
                pivot_stage(q, kb + 1)

    def begin(q):
        state_s[0] = 0
        state_s[1] = 0
        pivot_stage(q, 0)

    def drain(q):
        def one_block(kb, c):
            position = state_s[1]

            def some(p, cc):
                for g in range(GROUP):
                    update(q, kb, plan_row[position + p * GROUP + g], plan_col[position + p * GROUP + g])
                return cc

            lax.fori_loop(0, (plan_start[kb + 1] - position) // GROUP, some, 0)
            state_s[1] = plan_start[kb + 1]

            @pl.when(kb + 1 < blocks)
            def _():
                pivot_stage(q, kb + 1)

            return c

        lax.fori_loop(state_s[0], blocks, one_block, 0)

    def one_batch(batch, carry):
        base = batch * SUB
        q = lax.rem(batch, 2)
        more = base + SUB < used

        @pl.when(batch == 0)
        def _():
            fill(batch)
            begin(q)

        drain(q)
        state_s[0] = blocks
        logs = jnp.zeros((SUB, LANES), jnp.float32)
        for i in range(n):
            d = pivots[pl.ds(i * SUB, SUB), :]
            roots[pl.ds(i * SUB, SUB), :] = lax.rsqrt(d)
            logs = logs + jnp.log(d)
        halfdet[...] = log_prior - 0.5 * logs
        head_forms(q)

        @pl.when(batch == 0)
        def _():
            fetch.wait()
            prepare(order_s[0], following)

        @pl.when(more)
        def _():
            fill(batch + 1)
            begin(1 - q)

        def one_slot(slot, c):
            s = slot - base
            for piece, part in enumerate(split3(forms[pl.ds(s, LANES, stride=SUB), :])[:2]):
                form_weights[pl.ds(piece * LANES, LANES), :] = part
            for i in range(HEAD, n):
                groups = min(i // 16 + 1, even // 16)
                rows = groups * 16
                root = roots[pl.ds(i * SUB + s, SUB, stride=0), :][0:1, :]
                row = table[pl.ds(q * (n + edge) * n * SUB + i * n * SUB + s, rows, stride=SUB), :]
                if i < even:
                    j = lax.broadcasted_iota(jnp.int32, (rows, LANES), 0)
                    row = jnp.where(j < i, row, jnp.where(j == i, 1.0, 0.0))
                row = row * root
                one = row.astype(jnp.bfloat16)
                two = (row - one.astype(jnp.float32)).astype(jnp.bfloat16)
                weights[i, pl.ds(0, rows), :] = one
                weights[i, pl.ds(even, rows), :] = two
                if i >= even:
                    first = root.astype(jnp.bfloat16)
                    second = (root - first.astype(jnp.float32)).astype(jnp.bfloat16)
                    j = lax.broadcasted_iota(jnp.int32, (16, LANES), 0)
                    tail = jnp.zeros((16, LANES), jnp.float32)
                    for piece, part in enumerate((first, first, second, second, first)):
                        tail = jnp.where(j == piece, part.astype(jnp.float32), tail)
                    weights[i, pl.ds(2 * even, 16), :] = tail.astype(jnp.bfloat16)
            row_const = halfdet[pl.ds(s, 1), :]

            def operand(i):
                one = weights[i, pl.ds(0, even), :]
                two = weights[i, pl.ds(even, even), :]
                return jnp.concatenate([one, one, two, two, one, weights[i, pl.ds(2 * even, 16), :]], axis=0)

            def one_tile(place_at, cc):
                before = order_s[jnp.maximum(place_at - 1, 0)]
                side = lax.rem(place_at, 2)

                @pl.when(place_at >= 3)
                def _():
                    store(0, 1 - side).wait()

                def body(beside):
                    flipped[...] = following[...]
                    prepare(order_s[place_at + 1], following)
                    conclude(before, 1 - side)
                    head_features(order_s[place_at])
                    for i in range(HEAD, n, 2):
                        right = jnp.concatenate([operand(r) for r in range(i, min(i + 2, n))], axis=1)
                        white = jnp.dot(flipped[...], right, preferred_element_type=jnp.float32)
                        square = white[:, :LANES] * white[:, :LANES]
                        if i + 1 < n:
                            square = square + white[:, LANES:] * white[:, LANES:]
                        if i > HEAD:
                            acc[...] += square
                        else:
                            acc[...] = square
                        if beside is not None:
                            for g in range(GROUP):
                                if (2 * g + 1) * (n - HEAD) // (2 * GROUP) // 2 == (i - HEAD) // 2:
                                    beside(g)
                    done[...] = row_const - 0.5 * (acc[...] + head_norm())

                kb = state_s[0]
                position = state_s[1]
                working = kb < blocks

                @pl.when(working)
                def _():
                    body(lambda g: update(1 - q, kb, plan_row[position + g], plan_col[position + g]))
                    state_s[1] = position + GROUP
                    advance(1 - q)

                @pl.when(jnp.logical_not(working))
                def _():
                    body(None)

                @pl.when(place_at >= 1)
                def _():
                    store(before, 1 - side).start()

                return cc

            lax.fori_loop(start_s[slot], start_s[slot + 1], one_tile, 0)
            return c

        lax.fori_loop(base, jnp.minimum(used, base + SUB), one_slot, 0)
        return carry

    lax.fori_loop(0, (used + SUB - 1) // SUB, one_batch, 0)
    last = order_s[tiles - 1]
    side = (tiles - 1) % 2
    if tiles >= 3:
        store(0, side).wait()
    conclude(last, side)
    store(last, side).start()
    if tiles >= 2:
        store(0, 1 - side).wait()
    store(last, side).wait()


def shifted_scores(effects, se_table, se_index, covar, grid_scale, comp_grid, weights):
    n, pairs = effects.shape
    patterns = se_table.shape[0]
    tiles = pairs // TILE
    even = n // 16 * 16
    assert covar.shape == (n * n, LANES) and (n - even) * PIECES <= 16
    depth = PIECES * even + 16
    edge = block_edge(n)
    plan = update_plan(n // edge, GROUP)
    vmem = pl.BlockSpec(memory_space=pltpu.VMEM)
    smem = pl.BlockSpec(memory_space=pltpu.SMEM)
    hbm = pl.BlockSpec(memory_space=pl.ANY)
    f32 = jnp.float32
    return pl.pallas_call(
        functools.partial(main_kernel, n, tiles, patterns, grid_scale.shape[0]),
        name="shifted_scores",
        out_shape=(
            jax.ShapeDtypeStruct((LANES, pairs), f32),
            jax.ShapeDtypeStruct((2, pairs), f32),
        ),
        in_specs=[smem] * 5 + [hbm, vmem, hbm, vmem, vmem],
        out_specs=(hbm, vmem),
        scratch_shapes=[
            pltpu.VMEM((2 * (n + edge) * n * SUB, LANES), f32),
            pltpu.VMEM((n * SUB, LANES), f32),
            pltpu.VMEM(((edge * n + edge) * SUB, LANES), f32),
            pltpu.VMEM((n * SUB, LANES), f32),
            pltpu.VMEM((SUB, LANES), f32),
            pltpu.VMEM((n * SUB, LANES), f32),
            pltpu.VMEM((n, 2 * even + 16, LANES), jnp.bfloat16),
            pltpu.VMEM((n, pairs), f32),
            pltpu.VMEM((n * n, LANES), f32),
            pltpu.VMEM((TILE, depth), jnp.bfloat16),
            pltpu.VMEM((TILE, depth), jnp.bfloat16),
            pltpu.VMEM((depth, TILE), f32),
            pltpu.VMEM((TILE, LANES), f32),
            pltpu.VMEM((TILE, LANES), f32),
            pltpu.VMEM((2, LANES, TILE), f32),
            pltpu.VMEM((SUB, n), f32),
            pltpu.VMEM((HEAD * HEAD * SUB, LANES), f32),
            pltpu.VMEM((LANES * SUB, LANES), f32),
            pltpu.VMEM((2 * LANES, LANES), jnp.bfloat16),
            pltpu.VMEM((2 * SPAN, TILE), f32),
            pltpu.VMEM((LANES, TILE), f32),
            pltpu.VMEM((TILE, 2 * LANES), jnp.bfloat16),
            pltpu.SemaphoreType.DMA,
            pltpu.SemaphoreType.DMA,
            pltpu.SemaphoreType.DMA((2,)),
            pltpu.SMEM((patterns + 1,), jnp.int32),
            pltpu.SMEM((patterns + 1,), jnp.int32),
            pltpu.SMEM((patterns + 1,), jnp.int32),
            pltpu.SMEM((tiles + 1,), jnp.int32),
            pltpu.SMEM((2,), jnp.int32),
        ],
        compiler_params=pltpu.CompilerParams(vmem_limit_bytes=40 * 1024 * 1024),
    )(se_index, grid_scale, *plan, effects, se_table, covar, comp_grid[None], weights[None])


def exact_dot(left, right, dims):
    return lax.dot_general(left, right, (dims, ((), ())), precision=lax.Precision.HIGHEST, preferred_element_type=jnp.float32)


def finish_kernel(width, shifted_ref, own_ref, peaks_ref, out_hbm, loglik_ref, mass_ref, buffer, sems):
    pairs = shifted_ref.shape[1]
    steps = pairs // width
    copies = []
    partial = None
    for step in range(steps):
        at = pl.ds(step * width, width)
        tops = [peaks_ref[c, 0:1, at] for c in range(peaks_ref.shape[0])]
        sums = [peaks_ref[c, 1:2, at] for c in range(peaks_ref.shape[0])]
        top = functools.reduce(jnp.maximum, tops)
        total = sum(s * jnp.exp(t - top) for s, t in zip(sums, tops))
        loglik = top + jnp.log(total)
        loglik_ref[:, at] = loglik
        factor = jnp.exp(own_ref[0:1, at] - loglik)
        for c in range(width // LANES):
            lanes = pl.ds(step * width + c * LANES, LANES)
            value = shifted_ref[:, lanes] * factor[:, c * LANES : (c + 1) * LANES]
            buffer[:, lanes] = value
            partial = value if partial is None else partial + value
        copy = pltpu.make_async_copy(buffer.at[:, at], out_hbm.at[:, at], sems.at[step])
        copy.start()
        copies.append(copy)
    mass = jnp.sum(jnp.transpose(partial), axis=0, keepdims=True)
    mass_ref[...] = jnp.broadcast_to(mass, mass_ref.shape)
    for copy in copies:
        copy.wait()


def finish(shifted, peak, peaks, receivers):
    comps, pairs = shifted.shape
    width = min(pairs, 1024)
    vmem = pl.BlockSpec(memory_space=pltpu.VMEM)
    return pl.pallas_call(
        functools.partial(finish_kernel, width),
        name="finish",
        in_specs=[vmem, vmem, vmem],
        out_specs=(pl.BlockSpec(memory_space=pl.ANY), vmem, vmem),
        out_shape=(
            jax.ShapeDtypeStruct((comps, pairs), jnp.float32),
            jax.ShapeDtypeStruct((1, pairs), jnp.float32),
            jax.ShapeDtypeStruct((receivers, comps), jnp.float32),
        ),
        scratch_shapes=[pltpu.VMEM((comps, pairs), jnp.float32), pltpu.SemaphoreType.DMA((pairs // width,))],
        compiler_params=pltpu.CompilerParams(vmem_limit_bytes=12 * 1024 * 1024),
    )(shifted, peak, peaks)


def per_device(effects, se_table, se_index, base_root, grid_scale, comp_base, comp_grid, weights):
    n, pairs = effects.shape
    comps = comp_base.shape[0]
    covariances = jnp.einsum("uij,ukj->uik", base_root, base_root, precision=lax.Precision.HIGHEST)
    covariances = covariances.reshape(covariances.shape[0], n * n)
    bases = jnp.arange(covariances.shape[0], dtype=jnp.int32)
    pick = (comp_base[None] == bases[:, None]).astype(jnp.float32)
    covar = exact_dot(covariances, pick, ((0,), (0,)))
    shifted, peak = shifted_scores(effects, se_table, se_index, covar, grid_scale, comp_grid, weights)
    peaks = lax.all_gather(peak, "comp")
    receivers = lax.axis_size("pairs")
    responsibility, loglik, mass = finish(shifted, peak, peaks, receivers)
    masses = jnp.sum(lax.all_to_all(mass, "pairs", 0, 0, tiled=True), axis=0)
    all_pairs = pairs * lax.axis_size("pairs")
    all_comps = comps * lax.axis_size("comp")
    log_weights = jnp.log((masses + 1.0) / (all_pairs + all_comps))
    return (responsibility, log_weights, loglik[0])


def solution(mesh):
    placed = (P(None, "pairs"), P(), P("pairs"), P(), P(), P("comp"), P("comp"), P("comp"))
    return jax.shard_map(
        per_device,
        mesh=mesh,
        in_specs=placed,
        out_specs=(P("comp", "pairs"), P("comp"), P("pairs")),
        check_vma=False,
    )
```
